256 devices in a mesh: dp: 4 (over y), expert: 64 (over x, z, core).
Axes of the slice: x: 4, y: 4, z: 8, core: 2. Of those that a mesh axis runs over, the one named last changes fastest.
Arguments:
- tokens: bfloat16 [32768, 4096], P(('dp', 'expert')), may hold values from -6 to 6
- routes: int32 [32768, 2], P(('dp', 'expert')), may hold values from 0 to 63, all different within a row; in each aligned block of 128 rows (0 to 127, 128 to 255, ...) at most 6 rows name the same one
- router_weight: bfloat16 [4096, 64], replicated, may hold values from -0.09375 to 0.09375
- shift: float32 [8, 4096], replicated, may hold values from -3 to 3
- scale: float32 [8, 4096], replicated, may hold values from -3 to 3
- gate_mod: float32 [8, 4096], replicated, may hold values from -4 to 4
- gate_weight: bfloat16 [64, 4096, 1024], P(None, ('dp', 'expert')), may hold values from -0.09375 to 0.09375
- up_weight: bfloat16 [64, 4096, 1024], P(None, ('dp', 'expert')), may hold values from -0.09375 to 0.09375
- down_weight: bfloat16 [64, 4096, 1024], P(None, ('dp', 'expert')), may hold values from -0.1875 to 0.1875
Outputs:
- update: bfloat16 [32768, 4096], P(('dp', 'expert'))
The draws below stay inside these ranges and needn't reach their ends.
Inputs may be any that keep to these rules, and one draw needn't show every extreme that they name: `routes`: each row names two different experts; among the rows of one device no expert is named more than 6 times, a bound that some block reaches.
All inputs are finite; a program needn't handle non-finite values.
Results may differ from the reference program's by a relative error of at most 0.0072.
Values may be sent and summed in bfloat16 or wider, within the bound.
A program may use at most 128 MiB of HBM per device.

```python
import math
import jax
import jax.numpy as jnp
import numpy as np
from jax import lax

D = 4096
FE = 1024
E = 64
TOK_DEV = 128
CAP = 6
PIX = 4096
TOKENS = 32768
IMAGES = 8


def steps_of(key, extent, cuts, least, high):
    level, own = 1.0, jax.random.fold_in(key, 6)
    for dim, blocks in cuts:
        steps = jnp.exp(jax.random.uniform(jax.random.fold_in(own, dim), (blocks,), jnp.float32, least / len(cuts), high / len(cuts)))
        level = level * jnp.repeat(steps, extent[dim] // blocks).reshape([-1 if axis == dim else 1 for axis in range(len(extent))])
    return level


def routed_block(rng, own, number, rows, count, top, limit, skew):
    order = jax.random.permutation(rng, count)
    crowded, usual = shares(count, rows * top, limit, skew, True), shares(count, rows * top, limit, skew, False)
    places = jnp.arange(count)

    def named(tallies, turn):
        used = int((tallies > 0).sum())
        fixed = max(1, used // 4)
        moved = fixed + (places - fixed + turn * (used - fixed)) % max(1, count - fixed)
        return jnp.zeros((count,), jnp.int32).at[order[jnp.where(places < fixed, places, moved)]].set(jnp.asarray(tallies, jnp.int32))

    tallies = jnp.where(number % 4 == 0, named(crowded, number // 4), named(usual, number - number // 4 - 1))
    mixed = jax.random.permutation(jax.random.fold_in(own, 3), count)
    donor, receiver = mixed[0:count // 2 * 2:2], mixed[1:count // 2 * 2:2]
    margin = jnp.minimum(tallies[donor] - 1, limit - tallies[receiver]) // 2
    margin = jnp.where((donor == order[0]) | (receiver == order[0]) | (tallies[receiver] == 0), 0, jnp.maximum(margin, 0))
    moved = jax.random.randint(jax.random.fold_in(own, 4), (count // 2,), 0, 1 << 20) % (margin + 1)
    tallies = tallies.at[donor].add(-moved).at[receiver].add(moved)
    labels = jnp.searchsorted(jnp.cumsum(tallies), jnp.arange(rows * top), side="right").astype(jnp.int32)
    listing = labels.reshape(top, rows).T
    listing = listing[jax.random.permutation(jax.random.fold_in(own, 1), rows)]
    turn = jax.random.randint(jax.random.fold_in(own, 2), (rows, 1), 0, top)
    return jnp.take_along_axis(listing, (jnp.arange(top)[None, :] + turn) % top, axis=1)


def shares(number_of, total, reach, lean, full):
    loads = [(1 << 20) // math.isqrt(rank ** lean) + 1 for rank in range(1, number_of + 1)]
    largest = reach if full else min(reach, max(-(-total // number_of), total * loads[0] // sum(loads)))
    least = 1 if total - largest >= number_of - 1 else 0
    given, rest = [largest] + [least] * (number_of - 1), total - largest - least * (number_of - 1)
    while rest > 0:
        candidates = [i for i in range(1, number_of) if given[i] < largest] or [i for i in range(1, number_of) if given[i] < reach]
        mass, budget = sum([loads[i] for i in candidates]), rest
        for i in candidates:
            addition = min(reach - given[i], max(1, budget * loads[i] // mass), rest)
            given[i] = given[i] + addition
            rest = rest - addition
    return np.array(given)


def gaussian(rng, shape, scale, bound, pieces=(), kind=jnp.bfloat16):
    factor_of = steps_of(rng, shape, pieces, -0.22, 0.18) if pieces else 1.0
    result = jax.random.normal(rng, shape, jnp.float32) * scale * factor_of
    return jnp.minimum(jnp.maximum(result, -bound), bound).astype(kind)


def setup_inputs(seed: int = 0) -> dict:
    arg_keys = jax.random.split(jax.random.key(seed), 10)
    tokens = gaussian(arg_keys[0], (TOKENS, D), 1.0, 6.0, ((0, 256),))
    routes_keys = jax.random.split(jax.random.fold_in(arg_keys[1], 1), TOKENS // TOK_DEV)
    routes_turns = jax.random.permutation(jax.random.fold_in(arg_keys[1], 3), TOKENS // TOK_DEV)
    routes = jax.vmap(lambda own, number: routed_block(jax.random.fold_in(arg_keys[1], 2), own, number, TOK_DEV, E, 2, CAP, 2))(routes_keys, routes_turns).reshape((TOKENS, 2))
    router_weight = gaussian(arg_keys[2], (D, E), D ** -0.5, 0.09375)
    shift = gaussian(arg_keys[3], (IMAGES, D), 0.5, 3.0, (), jnp.float32)
    scale = gaussian(arg_keys[4], (IMAGES, D), 0.5, 3.0, (), jnp.float32)
    gate_mod = gaussian(arg_keys[5], (IMAGES, D), 1.0, 4.0, (), jnp.float32)
    gate_weight = gaussian(arg_keys[6], (E, D, FE), D ** -0.5, 0.09375, ((1, 256),))
    up_weight = gaussian(arg_keys[7], (E, D, FE), D ** -0.5, 0.09375, ((1, 256),))
    down_weight = gaussian(arg_keys[8], (E, D, FE), FE ** -0.5, 0.1875, ((1, 256),))
    return dict(tokens=tokens, routes=routes, router_weight=router_weight, shift=shift, scale=scale, gate_mod=gate_mod, gate_weight=gate_weight, up_weight=up_weight, down_weight=down_weight)


EPS = 1e-06

def reference(tokens, routes, router_weight, shift, scale, gate_mod, gate_weight, up_weight, down_weight):
    blocks = TOKENS // TOK_DEV

    def norm_image(items):
        rows, image_shift, image_scale = items
        values = rows.astype(jnp.float32)
        meansq = lax.optimization_barrier(jnp.mean(values * values, axis=-1, keepdims=True))
        normed_rows = values * lax.rsqrt(meansq + EPS) * (1.0 + image_scale[None, :]) + image_shift[None, :]
        normed_rows = normed_rows.astype(jnp.bfloat16)
        logit_rows = jnp.dot(normed_rows, router_weight, preferred_element_type=jnp.float32)
        return (normed_rows, logit_rows)
    normed, logits = lax.map(norm_image, (tokens.reshape(IMAGES, PIX, D), shift, scale))
    normed = normed.reshape(TOKENS, D)
    logits = logits.reshape(TOKENS, E)
    chosen = jnp.take_along_axis(logits, routes, axis=1)
    score_flat = jax.nn.sigmoid(chosen).reshape(-1)
    flat = routes.reshape(blocks, 2 * TOK_DEV)
    hot = (flat[:, :, None] == jnp.arange(E, dtype=jnp.int32)[None, None, :]).astype(jnp.int32)
    rank = (jnp.cumsum(hot, axis=1) - hot).astype(jnp.int32)
    slot = lax.optimization_barrier(jnp.sum(rank * hot, axis=-1)).astype(jnp.int32)
    position = (flat * CAP + slot).astype(jnp.int32)
    global_ids = (jnp.arange(blocks, dtype=jnp.int32)[:, None] * (2 * TOK_DEV) + jnp.arange(2 * TOK_DEV, dtype=jnp.int32)[None, :]).astype(jnp.int32)

    def fill_table(where_to, ids):
        return jnp.full((E * CAP,), -1, jnp.int32).at[where_to].set(ids)
    table = jax.vmap(fill_table)(position, global_ids)
    table = table.reshape(blocks, E, CAP).transpose(1, 0, 2).reshape(E, blocks * CAP)

    def expert_step(total, items):
        ids, w_gate, w_up, w_down = items
        filled = ids >= 0
        safe = jnp.where(filled, ids, 0).astype(jnp.int32)
        token_ids = (safe // 2).astype(jnp.int32)
        rows = jnp.where(filled[:, None], normed[token_ids], jnp.zeros((), jnp.bfloat16))
        gate = jnp.dot(rows, w_gate, preferred_element_type=jnp.float32)
        upper = jnp.dot(rows, w_up, preferred_element_type=jnp.float32)
        hidden = (jax.nn.silu(gate) * upper).astype(jnp.bfloat16)
        output = jnp.dot(hidden, w_down.T, preferred_element_type=jnp.float32).astype(jnp.bfloat16)
        weight = jnp.where(filled, score_flat[safe], jnp.zeros((), jnp.float32))
        total = total.at[token_ids].add(weight[:, None] * output.astype(jnp.float32))
        return (total, None)
    total, unused = lax.scan(expert_step, jnp.zeros((TOKENS, D), jnp.float32), (table, gate_weight, up_weight, down_weight))
    update = total.reshape(IMAGES, PIX, D) * gate_mod[:, None, :]
    return update.reshape(TOKENS, D).astype(jnp.bfloat16)
```

```python
import functools

import jax
import jax.numpy as jnp
import numpy as np
from jax import lax
from jax.experimental import pallas as pl
from jax.experimental.pallas import tpu as pltpu
from jax.sharding import PartitionSpec as P

MESH = pl.DeviceIdType.MESH
PIX = 4096
EPS = 1e-06
NX, NZ, NC, NY = 4, 8, 2, 4
N = NX * NZ * NC
CAP = 6
BLK = 512
NB = 8
ROWS = NB * CAP
GRP = 8
WIN = 16
LAG = 4
TLAG = 9
ROT = 20
F32, BF16 = jnp.float32, jnp.bfloat16


def offset(k):
    k = lax.rem(k + ROT, N)
    q, m = lax.div(k, 8), lax.rem(k, 8)
    dz = lax.rem(m * 5 + 4, NZ)
    dx = lax.rem(q + 2 * m + lax.div(m, 2), NX)
    dc = lax.rem(lax.div(q, 4) + m, NC)
    return dx, dz, dc


def kernel(
    tok, routes, router, shift, scale, gmod, perm, gate, up, down, out,
    W, NBUF, SB, RB, IB, XB, H, PICK, SCORE,
    sA, sP, sM, sR, sT, sO, sL, rA, rP, rM, rC, rT, rR,
):
    e = lax.axis_index("expert")
    y = lax.axis_index("dp")
    x, z, c = lax.div(e, NZ * NC), lax.rem(lax.div(e, NC), NZ), lax.rem(e, NC)
    yp, ym, y2 = lax.rem(y + 1, NY), lax.rem(y + 3, NY), lax.rem(y + 2, NY)

    def tgt(k):
        dx, dz, dc = offset(k)
        return (lax.rem(x + dx, NX) * NZ + lax.rem(z + dz, NZ)) * NC + lax.rem(c + dc, NC)

    def src(k):
        dx, dz, dc = offset(k)
        return (lax.rem(x + NX - dx, NX) * NZ + lax.rem(z + NZ - dz, NZ)) * NC + lax.rem(c + dc, NC)

    def loop(lo, hi, f):
        def body(k, carry):
            f(k)
            return carry
        lax.fori_loop(lo, hi, body, 0)

    bar = pltpu.get_barrier_semaphore()
    loop(1, N, lambda k: pl.semaphore_signal(bar, 1, device_id=(y, tgt(k)), device_id_type=MESH))
    pl.semaphore_signal(bar, 1, device_id=(yp, e), device_id_type=MESH)
    pl.semaphore_signal(bar, 1, device_id=(ym, e), device_id_type=MESH)
    pl.semaphore_wait(bar, N + 1)

    weights = (gate, up, down)

    def send_w(k):
        t = tgt(k)
        for j in range(3):
            pltpu.make_async_remote_copy(
                weights[j].at[t], W.at[y * N + e, j], sA, rA.at[k],
                device_id=(y, t), device_id_type=MESH,
            ).start()

    def chunk(i, s, r, device):
        return pltpu.make_async_remote_copy(
            W.at[i], W.at[i], s, r, device_id=device, device_id_type=MESH
        )

    def send_t(k):
        return pltpu.make_async_remote_copy(
            SB.at[k], RB.at[k], sT, rT.at[k], device_id=(y, tgt(k)), device_id_type=MESH
        )

    def send_o(k):
        return pltpu.make_async_remote_copy(
            SB.at[k], IB.at[k], sO, rR.at[k], device_id=(y, src(k)), device_id_type=MESH
        )

    for j in range(3):
        pltpu.make_async_copy(weights[j].at[e], W.at[y * N + e, j], sL).start()
    loop(1, WIN, send_w)

    image = lax.div((y * N + e) * tok.shape[0], PIX)
    square = jnp.zeros((tok.shape[0], 1), F32)
    for j in range(NB):
        v = tok[:, j * BLK:(j + 1) * BLK].astype(F32)
        square = square + jnp.sum(v * v, axis=-1, keepdims=True)
    inv = lax.rsqrt(square * (1.0 / (NB * BLK)) + EPS)
    logits = jnp.zeros((tok.shape[0], N), F32)
    for j in range(NB):
        cols = slice(j * BLK, (j + 1) * BLK)
        v = tok[:, cols].astype(F32)
        normed = v * inv * (1.0 + scale[pl.ds(image, 1), cols]) + shift[pl.ds(image, 1), cols]
        normed = normed.astype(BF16)
        NBUF[j] = normed
        logits = logits + jnp.dot(normed, router[cols, :], preferred_element_type=F32)
    tokens = tok.shape[0]
    experts = lax.broadcasted_iota(jnp.int32, (tokens, N), 1)
    named = [routes[:, k:k + 1] for k in range(2)]
    hot = [(experts == named[k]).astype(F32) for k in range(2)]
    below = (
        lax.broadcasted_iota(jnp.int32, (tokens, tokens), 1)
        < lax.broadcasted_iota(jnp.int32, (tokens, tokens), 0)
    ).astype(F32).astype(BF16)
    earlier = jnp.dot(below, (hot[0] + hot[1]).astype(BF16), preferred_element_type=F32)
    places = lax.broadcasted_iota(jnp.int32, (tokens, N * CAP), 1)
    both = None
    for k in range(2):
        r = named[k]
        ex, ez, ec = r >> 4, (r >> 1) & 7, r & 1
        dx, dz, dc = (ex - x + NX) & 3, (ez - z + NZ) & 7, (ec + c) & 1
        m = (dz * 5 + 4) & 7
        q = ((dx - 2 * m - (m >> 1) + 32) & 3) + 4 * ((dc + m) & 1)
        step = (8 * q + m + N - ROT) & (N - 1)
        slot = jnp.sum(hot[k] * earlier, axis=-1, keepdims=True).astype(jnp.int32)
        pick = (places == step * CAP + slot).astype(F32)
        PICK[k] = pick.astype(BF16)
        both = pick if both is None else both + pick
        chosen = jnp.sum(hot[k] * logits, axis=-1, keepdims=True)
        SCORE[k] = jnp.broadcast_to(jax.nn.sigmoid(chosen), (tokens, 128))
    select = both.T.astype(BF16)

    def gather_rows(j):
        XB[j] = jnp.dot(select, NBUF[j], preferred_element_type=F32).astype(BF16)
    loop(0, NB, gather_rows)

    def to_wire(g):
        rows = pl.ds(pl.multiple_of(g * ROWS, 16), ROWS)
        block = XB[:, rows, :].reshape(NB * ROWS, BLK)
        moved = jnp.dot(perm[...], block, preferred_element_type=F32).astype(BF16)
        SB[pl.ds(g * GRP, GRP)] = moved.reshape(GRP, ROWS, BLK)

    def from_wire(buf, g):
        rows = pl.ds(pl.multiple_of(g * ROWS, 16), ROWS)
        block = buf[pl.ds(g * GRP, GRP)].reshape(GRP * ROWS, BLK)
        moved = jnp.dot(perm[...], block, preferred_element_type=F32).astype(BF16)
        XB[:, rows, :] = moved.reshape(NB, ROWS, BLK)

    mine = W.at[y * N + e]
    pltpu.make_async_copy(mine, mine, sL).wait()

    def forward(k):
        i = y * N + src(k)
        chunk(i, sP, rP.at[k], (yp, e)).start()
        chunk(i, sM, rM.at[k], (ym, e)).start()

    def relay(k):
        s = src(k)

        def up_way():
            i = ym * N + s
            chunk(i, sP, rP.at[k], (yp, e)).wait_recv()
            chunk(i, sR, rC.at[k], (yp, e)).start()

        def down_way():
            i = yp * N + s
            chunk(i, sM, rM.at[k], (ym, e)).wait_recv()
            chunk(i, sR, rC.at[k], (ym, e)).start()

        lax.cond(lax.rem(k, 2) == 0, up_way, down_way)

    forward(0)

    def step(k):
        @pl.when(k + WIN - 1 < N)
        def _():
            send_w(k + WIN - 1)

        @pl.when(k <= N // GRP)
        def _():
            to_wire(k - 1)

        @pl.when(k > TLAG)
        def _():
            send_t(k - TLAG).start()

        chunk(y * N + src(k), sA, rA.at[k], (y, e)).wait_recv()
        forward(k)

        @pl.when(k >= LAG)
        def _():
            relay(k - LAG)

    loop(1, N, step)
    loop(N - TLAG, N, lambda k: send_t(k).start())
    loop(N - LAG, N, relay)
    RB[0] = SB[0]

    def last(k):
        s = src(k)

        def odd_way():
            chunk(yp * N + s, sM, rM.at[k], (ym, e)).wait_recv()

        def even_way():
            chunk(ym * N + s, sP, rP.at[k], (yp, e)).wait_recv()

        lax.cond(lax.rem(k, 2) == 0, odd_way, even_way)
        chunk(y2 * N + s, sR, rC.at[k], (yp, e)).wait_recv()

    loop(1, N, lambda k: send_t(k).wait_recv())
    loop(0, N // GRP, lambda g: from_wire(RB, g))
    loop(0, N, last)

    def hidden(n):
        cols = pl.ds(pl.multiple_of(n * 256, 256), 256)
        g = u = None
        for j in range(NB):
            rows = slice(j * 32, (j + 1) * 32)
            a = XB[j]
            pg = jnp.dot(a, W[rows, 0, :, cols].reshape(BLK, 256), preferred_element_type=F32)
            pu = jnp.dot(a, W[rows, 1, :, cols].reshape(BLK, 256), preferred_element_type=F32)
            g, u = (pg, pu) if g is None else (g + pg, u + pu)
        H[:, cols] = (g / (1.0 + jnp.exp(-g)) * u).astype(BF16)
    loop(0, 4, hidden)

    def outputs(j):
        wd = W[pl.ds(j * 32, 32), 2].reshape(BLK, 1024)
        o = lax.dot_general(H[...], wd, (((1,), (1,)), ((), ())), preferred_element_type=F32)
        XB[j] = o.astype(BF16)
    loop(0, NB, outputs)

    rest = SB.at[pl.ds(1, N - 1)]
    pltpu.make_async_remote_copy(rest, rest, sT, sL, device_id=(y, e), device_id_type=MESH).wait_send()

    def back(g):
        to_wire(g)

        @pl.when(g == 0)
        def _():
            IB[0] = SB[0]

        @pl.when(g > 0)
        def _():
            loop(0, GRP, lambda i: send_some(g * GRP - GRP + i))

    def send_some(k):
        @pl.when(k > 0)
        def _():
            send_o(k).start()

    loop(0, N // GRP, back)
    loop(N - GRP, N, lambda k: send_o(k).start())

    def come(g):
        def one(k):
            @pl.when(k > 0)
            def _():
                send_o(k).wait_recv()
        loop(g * GRP, g * GRP + GRP, one)
        from_wire(IB, g)

    loop(0, N // GRP, come)

    for j in range(NB):
        cols = slice(j * BLK, (j + 1) * BLK)
        block = XB[j]
        total = None
        for k in range(2):
            part = jnp.dot(PICK[k], block, preferred_element_type=F32) * SCORE[k][:, 0:1]
            total = part if total is None else total + part
        out[:, cols] = (gmod[pl.ds(image, 1), cols] * total).astype(BF16)

    pltpu.make_async_remote_copy(rest, rest, sO, sL, device_id=(y, e), device_id_type=MESH).wait_send()
    most = W.at[pl.ds(0, N - 1)]
    pltpu.make_async_remote_copy(most, most, sA, sL, device_id=(y, e), device_id_type=MESH).wait_send()
    full = W.at[pl.ds(0, N)]
    for s in (sP, sM, sR):
        pltpu.make_async_remote_copy(full, full, s, sL, device_id=(y, e), device_id_type=MESH).wait_send()


def permutation():
    p = np.zeros((NB * ROWS, GRP * ROWS), np.float32)
    for a in range(GRP):
        for j in range(NB):
            for r in range(CAP):
                p[a * ROWS + j * CAP + r, j * ROWS + a * CAP + r] = 1.0
    return p


def shards(tokens, routes, router_weight, shift, scale, gate_mod, gate_weight, up_weight, down_weight):
    rows, width = tokens.shape
    perm = jnp.asarray(permutation(), BF16)
    D = pltpu.SemaphoreType.DMA
    V = pltpu.VMEM
    vmem = pl.BlockSpec(memory_space=pltpu.VMEM)
    hbm = pl.BlockSpec(memory_space=pl.ANY)
    return pl.pallas_call(
        kernel,
        name="experts",
        out_shape=jax.ShapeDtypeStruct((rows, width), BF16),
        in_specs=[vmem] * 7 + [hbm] * 3,
        out_specs=vmem,
        scratch_shapes=[
            V((NY * N, 3, 16, 1024), BF16),
            V((NB, rows, BLK), BF16),
            V((N, ROWS, BLK), BF16),
            V((N, ROWS, BLK), BF16),
            V((N, ROWS, BLK), BF16),
            V((NB, N * CAP, BLK), BF16),
            V((N * CAP, 1024), BF16),
            V((2, rows, N * CAP), BF16),
            V((2, rows, 128), F32),
        ] + [D] * 7 + [D((N,))] * 6,
        compiler_params=pltpu.CompilerParams(
            collective_id=0, has_side_effects=True, vmem_limit_bytes=63 * 2**20
        ),
    )(tokens, routes, router_weight, shift, scale, gate_mod, perm, gate_weight, up_weight, down_weight)


def solution(mesh):
    spread = ("dp", "expert")
    in_specs = (
        P(spread, None), P(spread, None), P(), P(), P(), P(),
        P(None, spread, None), P(None, spread, None), P(None, spread, None),
    )
    return jax.shard_map(shards, mesh=mesh, in_specs=in_specs, out_specs=P(spread, None), check_vma=False)
```

```python
import functools

import jax
import jax.numpy as jnp
import numpy as np
from jax import lax
from jax.experimental import pallas as pl
from jax.experimental.pallas import tpu as pltpu
from jax.sharding import PartitionSpec as P

MESH = pl.DeviceIdType.MESH
PIX = 4096
EPS = 1e-06
NX, NZ, NC, NY = 4, 8, 2, 4
N = NX * NZ * NC
CAP = 6
BLK = 512
NB = 8
ROWS = NB * CAP
GRP = 8
NG = N // GRP
HALF = 256
NQ = NX * NZ
LAG = 4
ROT = 20
F32, BF16 = jnp.float32, jnp.bfloat16


def place(k):
    q = lax.rem(k + ROT, NQ)
    a, m = lax.div(q, 8), lax.rem(q, 8)
    dz = lax.rem(m * 5 + 4, NZ)
    dx = lax.rem(a + 2 * m + lax.div(m, 2), NX)
    return dx, dz, lax.div(k, NQ)


def kernel(
    tok_hbm, routes_hbm, router_hbm, shift_hbm, scale_hbm, gmod_hbm, perm_hbm, weave_hbm,
    gate, up, down, out,
    tok, routes, router, shift, scale, gmod, perm, weave, WG, WD, NBUF, SB, RB, XB, H, OUT, OB, IB, YB, PICK, SCORE, GP,
    sG, sGY, sD, sDY, sT, sO, sL, rG, rGP, rGM, rGR, rD, rDP, rDM, rDR, rT, rO, sI,
):
    e = lax.axis_index("expert")
    y = lax.axis_index("dp")
    x, z, c = lax.div(e, NZ * NC), lax.rem(lax.div(e, NC), NZ), lax.rem(e, NC)
    yp, ym, y2 = lax.rem(y + 1, NY), lax.rem(y + 3, NY), lax.rem(y + 2, NY)
    above, below = (yp, e), (ym, e)

    def chip(dx, dz):
        return lax.rem(x + dx, NX) * NZ + lax.rem(z + dz, NZ)

    def tgt(k):
        dx, dz, dc = place(k)
        return chip(dx, dz) * NC + lax.rem(c + dc, NC)

    def src(k):
        dx, dz, dc = place(k)
        return chip(NX - dx, NZ - dz) * NC + lax.rem(c + dc, NC)

    def loop(lo, hi, f):
        def body(k, carry):
            f(k)
            return carry
        lax.fori_loop(lo, hi, body, 0)

    def copy(a, b, s, r, device):
        return pltpu.make_async_remote_copy(a, b, s, r, device_id=device, device_id_type=MESH)

    bar = pltpu.get_barrier_semaphore()
    loop(1, N, lambda k: pl.semaphore_signal(bar, 1, device_id=(y, tgt(k)), device_id_type=MESH))
    pl.semaphore_signal(bar, 1, device_id=above, device_id_type=MESH)
    pl.semaphore_signal(bar, 1, device_id=below, device_id_type=MESH)
    small = (
        (tok_hbm, tok), (routes_hbm, routes), (router_hbm, router), (shift_hbm, shift),
        (scale_hbm, scale), (gmod_hbm, gmod), (perm_hbm, perm), (weave_hbm, weave),
    )
    loads = [pltpu.make_async_copy(a, b, sI.at[i]) for i, (a, b) in enumerate(small)]
    for load in loads:
        load.start()
    pl.semaphore_wait(bar, N + 1)

    def send_g(k):
        t = tgt(k)
        copy(gate.at[t], WG.at[y * N + e, 0], sG, rG.at[k], (y, t)).start()
        copy(up.at[t], WG.at[y * N + e, 1], sG, rG.at[k], (y, t)).start()

    mine_g = WG.at[y * N + e]
    mine_d = WD.at[c * NY * NQ + y * NQ + lax.div(e, NC)]
    pltpu.make_async_copy(gate.at[e], WG.at[y * N + e, 0], sL).start()
    pltpu.make_async_copy(up.at[e], WG.at[y * N + e, 1], sL).start()
    loop(1, N, send_g)
    pltpu.make_async_copy(mine_g, mine_g, sL).wait()
    pltpu.make_async_copy(down.at[e], mine_d, sL).start()

    def send_d(k):
        t = tgt(k)
        copy(down.at[t], mine_d, sD, rD.at[k], (y, t)).start()

    loop(1, NQ, send_d)
    pltpu.make_async_copy(mine_d, mine_d, sL).wait()

    for load in loads:
        load.wait()
    count = tok.shape[0]
    image = lax.div((y * N + e) * count, PIX)
    square = jnp.zeros((count, 1), F32)
    for j in range(NB):
        v = tok[:, j * BLK:(j + 1) * BLK].astype(F32)
        square = square + jnp.sum(v * v, axis=-1, keepdims=True)
    inv = lax.rsqrt(square * (1.0 / (NB * BLK)) + EPS)
    logits = jnp.zeros((count, N), F32)
    for j in range(NB):
        cols = slice(j * BLK, (j + 1) * BLK)
        v = tok[:, cols].astype(F32)
        normed = v * inv * (1.0 + scale[pl.ds(image, 1), cols]) + shift[pl.ds(image, 1), cols]
        normed = normed.astype(BF16)
        NBUF[j] = normed
        logits = logits + lax.dot_general(
            normed, router[:, cols], (((1,), (1,)), ((), ())), preferred_element_type=F32
        )
    experts = lax.broadcasted_iota(jnp.int32, (count, N), 1)
    tall = jnp.concatenate([routes[...].astype(F32), jnp.zeros((6, count), F32)], axis=0).T
    named = [tall[:, k:k + 1].astype(jnp.int32) for k in range(2)]
    hot = [(experts == named[k]).astype(F32) for k in range(2)]
    before = (
        lax.broadcasted_iota(jnp.int32, (count, count), 1)
        < lax.broadcasted_iota(jnp.int32, (count, count), 0)
    ).astype(F32).astype(BF16)
    earlier = jnp.dot(before, (hot[0] + hot[1]).astype(BF16), preferred_element_type=F32)
    places = lax.broadcasted_iota(jnp.int32, (count, N * CAP), 1)
    both = None
    for k in range(2):
        r = named[k]
        ex, ez, ec = r >> 4, (r >> 1) & 7, r & 1
        dx, dz, dc = (ex - x + NX) & 3, (ez - z + NZ) & 7, (ec + c) & 1
        m = (dz * 5 + 4) & 7
        a = (dx - 2 * m - (m >> 1) + 32) & 3
        step = ((8 * a + m + NQ - ROT) & (NQ - 1)) + NQ * dc
        slot = jnp.sum(hot[k] * earlier, axis=-1, keepdims=True).astype(jnp.int32)
        pick = (places == step * CAP + slot).astype(F32)
        PICK[k] = pick.astype(BF16)
        both = pick if both is None else both + pick
        chosen = jnp.sum(hot[k] * logits, axis=-1, keepdims=True)
        SCORE[k] = jnp.broadcast_to(jax.nn.sigmoid(chosen), (count, 128))
    select = both.T.astype(BF16)

    def gather_rows(j):
        XB[j] = jnp.dot(select, NBUF[j], preferred_element_type=F32).astype(BF16)
    loop(0, NB, gather_rows)

    for j in range(NB):
        left = gmod[pl.ds(image, 1), j * BLK:(j + 1) * BLK]
        terms = []
        for _ in range(3):
            term = left.astype(BF16)
            terms.append(term.astype(F32))
            left = left - terms[-1]
        stack = jnp.concatenate(terms + [jnp.zeros((5, BLK), F32)], axis=0).astype(BF16)
        moved = lax.dot_general(stack, weave[...], (((1,), (1,)), ((), ())), preferred_element_type=F32)
        GP[j:j + 1] = moved[0:1] + moved[1:2] + moved[2:3]

    def rows_of(g):
        return pl.ds(pl.multiple_of(g * ROWS, 16), ROWS)

    def turn(block):
        return jnp.dot(perm[...], block, preferred_element_type=F32).astype(BF16)

    def pack(g):
        block = turn(XB[:, rows_of(g), :].reshape(NB * ROWS, BLK))
        SB[pl.ds(g * GRP, GRP)] = block.reshape(GRP, ROWS, BLK)

    def unpack(g):
        block = turn(RB[pl.ds(g * GRP, GRP)].reshape(GRP * ROWS, BLK))
        XB[:, rows_of(g), :] = block.reshape(NB, ROWS, BLK)

    def send_t(k):
        copy(SB.at[k], RB.at[k], sT, rT.at[lax.div(k, GRP)], (y, tgt(k))).start()

    def forward_g(k):
        w = WG.at[y * N + src(k)]
        copy(w, w, sGY, rGP.at[k], above).start()
        copy(w, w, sGY, rGM.at[k], below).start()

    def up_g(k):
        w = WG.at[ym * N + src(k)]
        copy(w, w, sGY, rGP.at[k], above).wait_recv()
        return w

    def down_g(k):
        w = WG.at[yp * N + src(k)]
        copy(w, w, sGY, rGM.at[k], below).wait_recv()
        return w

    def far_g(k):
        w = WG.at[y2 * N + src(k)]
        copy(w, w, sGY, rGR.at[k], above).wait_recv()

    def relay_g(k):
        def one():
            w = up_g(k)
            copy(w, w, sGY, rGR.at[k], above).start()

        def two():
            w = down_g(k)
            copy(w, w, sGY, rGR.at[k], below).start()

        lax.cond(lax.rem(k, 2) == 0, one, two)

    def last_g(k):
        def one():
            down_g(k)

        def two():
            up_g(k)

        lax.cond(lax.rem(k, 2) == 0, one, two)
        far_g(k)

    forward_g(0)

    def step_g(k):
        @pl.when(k <= NG)
        def _():
            pack(k - 1)

        @pl.when((k >= 3) & (k < NG + 3))
        def _():
            first = (k - 3) * GRP
            loop(first, first + GRP, some_t)

        @pl.when(k == NG + 3)
        def _():
            loop(NQ, N, send_d)

        w = WG.at[y * N + src(k)]
        copy(w, w, sG, rG.at[k], above).wait_recv()
        forward_g(k)

        @pl.when(k >= LAG)
        def _():
            relay_g(k - LAG)

    def some_t(k):
        @pl.when(k > 0)
        def _():
            send_t(k)

    loop(1, N, step_g)
    loop(N - LAG, N, relay_g)
    RB[0] = SB[0]

    def class_of(phase):
        return lax.rem(c + phase, NC)

    def down_at(plane, k):
        return WD.at[class_of(lax.div(k, NQ)) * NY * NQ + plane * NQ + lax.div(src(k), NC)]

    def forward_d(k):
        w = down_at(y, k)

        @pl.when(k > 0)
        def _():
            copy(w, w, sD, rD.at[k], above).wait_recv()

        copy(w, w, sDY, rDP.at[k], above).start()
        copy(w, w, sDY, rDM.at[k], below).start()

    def up_d(k):
        w = down_at(ym, k)
        copy(w, w, sDY, rDP.at[k], above).wait_recv()
        return w

    def down_d(k):
        w = down_at(yp, k)
        copy(w, w, sDY, rDM.at[k], below).wait_recv()
        return w

    def relay_d(k):
        def one():
            w = up_d(k)
            copy(w, w, sDY, rDR.at[k], above).start()

        def two():
            w = down_d(k)
            copy(w, w, sDY, rDR.at[k], below).start()

        lax.cond(lax.rem(k, 2) == 0, one, two)

    def last_d(k):
        def one():
            down_d(k)

        def two():
            up_d(k)

        lax.cond(lax.rem(k, 2) == 0, one, two)
        w = down_at(y2, k)
        copy(w, w, sDY, rDR.at[k], above).wait_recv()

    def step_d(k):
        forward_d(k)

        @pl.when(k >= LAG)
        def _():
            relay_d(k - LAG)

    def hidden(n):
        cols = pl.ds(pl.multiple_of(n * 256, 256), 256)
        g = u = None
        for j in range(NB):
            rows = slice(j * 32, (j + 1) * 32)
            a = XB[j]
            pg = jnp.dot(a, WG[rows, 0, :, cols].reshape(BLK, 256), preferred_element_type=F32)
            pu = jnp.dot(a, WG[rows, 1, :, cols].reshape(BLK, 256), preferred_element_type=F32)
            g, u = (pg, pu) if g is None else (g + pg, u + pu)
        H[:, cols] = (g / (1.0 + jnp.exp(-g)) * u).astype(BF16)

    def send_o(kind, k):
        copy(
            OB.at[kind * N + k], IB.at[kind * N + k], sO,
            rO.at[kind * NG + lax.div(k, GRP)], (y, src(k)),
        ).start()

    def multiply(phase, also):
        kind = class_of(phase)

        def block(j):
            wd = WD[pl.ds(kind * NY * NQ + j * 16, 16)].reshape(HALF, 1024)
            o = lax.dot_general(H[...], wd, (((1,), (1,)), ((), ())), preferred_element_type=F32)
            OUT[j] = o.astype(BF16)
            also(j)
        loop(0, NB, block)

    def send_back(phase, also):
        kind = class_of(phase)

        def group(g):
            block = turn(OUT[:, rows_of(g), :].reshape(NB * ROWS, HALF))
            OB[pl.ds(kind * N + g * GRP, GRP)] = block.reshape(GRP, ROWS, HALF)

            @pl.when(g > 0)
            def _():
                loop(g * GRP - GRP, g * GRP, some)

            also(g)

        def some(k):
            @pl.when(k > 0)
            def _():
                send_o(kind, k)

        loop(0, NG, group)
        loop(N - GRP, N, some)
        IB[kind * N] = OB[kind * N]

    def collect(phase):
        def group(g):
            kind = lax.rem(c + phase + lax.div(g, NG // 2), NC)

            def wait(first, size):
                there = IB.at[pl.ds(kind * N + first, size)]
                copy(there, there, sO, rO.at[kind * NG + g], above).wait_recv()

            lax.cond(g == 0, lambda: wait(1, GRP - 1), lambda: wait(g * GRP, GRP))
            block = turn(IB[pl.ds(kind * N + g * GRP, GRP)].reshape(GRP * ROWS, HALF))
            YB[pl.ds(kind * NB, NB), rows_of(g), :] = block.reshape(NB, ROWS, HALF)
        loop(0, NG, group)

    def combine(j):
        parts = []
        for kind in range(NC):
            block = YB[kind * NB + j]
            total = None
            for k in range(2):
                part = jnp.dot(PICK[k], block, preferred_element_type=F32) * SCORE[k][:, 0:1]
                total = part if total is None else total + part
            parts.append((GP[j:j + 1, kind * HALF:(kind + 1) * HALF] * total).astype(BF16))
        both = jnp.concatenate(parts, axis=1)
        out[:, j * BLK:(j + 1) * BLK] = jnp.dot(both, weave[...], preferred_element_type=F32).astype(BF16)

    def hidden_and_pass(n):
        hidden(n)
        loop(NQ + 4 * n, NQ + 4 * n + 4, forward_d)

    def pass_more(j):
        forward_d(NQ + 16 + j)
        relay_d(NQ + j)

    def pass_most(g):
        forward_d(NQ + 24 + g)
        relay_d(NQ + 8 + g)

    def nothing(_):
        pass

    loop(0, NQ, step_d)
    loop(NQ - LAG, NQ, relay_d)
    for g in range(NG):
        there = RB.at[pl.ds(max(1, g * GRP), GRP - (g == 0))]
        copy(there, there, sT, rT.at[g], above).wait_recv()
    loop(0, NG, unpack)
    loop(0, N, last_g)
    loop(0, 4, hidden_and_pass)
    loop(0, NQ, last_d)
    multiply(0, pass_more)
    send_back(0, pass_most)
    loop(N - NQ // 2, N, relay_d)
    loop(NQ, N, last_d)
    multiply(1, nothing)
    send_back(1, nothing)
    collect(0)
    collect(1)
    for j in range(NB):
        combine(j)

    def left(ref, size, s):
        view = ref.at[pl.ds(0, size)]
        copy(view, view, s, sL, above).wait_send()

    left(WG, N - 1, sG)
    left(WG, 3 * N, sGY)
    left(WD, N - 1, sD)
    left(WD, 3 * N, sDY)
    left(SB, N - 1, sT)
    left(OB, 2 * N - 2, sO)


def permutation():
    p = np.zeros((NB * ROWS, GRP * ROWS), np.float32)
    for a in range(GRP):
        for j in range(NB):
            for r in range(CAP):
                p[a * ROWS + j * CAP + r, j * ROWS + a * CAP + r] = 1.0
    return p


def weaving():
    p = np.zeros((BLK, BLK), np.float32)
    for core in range(2):
        for s in range(16):
            for i in range(16):
                p[core * HALF + s * 16 + i, s * 32 + core * 16 + i] = 1.0
    return p


def shards(tokens, routes, router_weight, shift, scale, gate_mod, gate_weight, up_weight, down_weight):
    rows, width = tokens.shape
    perm, weave = jnp.asarray(permutation(), BF16), jnp.asarray(weaving(), BF16)
    small = (tokens, routes.T, router_weight.T, shift, scale, gate_mod, perm, weave)
    D = pltpu.SemaphoreType.DMA
    V = pltpu.VMEM
    vmem = pl.BlockSpec(memory_space=pltpu.VMEM)
    hbm = pl.BlockSpec(memory_space=pl.ANY)
    return pl.pallas_call(
        kernel,
        name="experts",
        out_shape=jax.ShapeDtypeStruct((rows, width), BF16),
        in_specs=[hbm] * 11,
        out_specs=vmem,
        scratch_shapes=[V(a.shape, a.dtype) for a in small] + [
            V((NY * N, 2, 16, 1024), BF16),
            V((NY * N, 16, 1024), BF16),
            V((NB, rows, BLK), BF16),
            V((N, ROWS, BLK), BF16),
            V((N, ROWS, BLK), BF16),
            V((NB, N * CAP, BLK), BF16),
            V((N * CAP, 1024), BF16),
            V((NB, N * CAP, HALF), BF16),
            V((2 * N, ROWS, HALF), BF16),
            V((2 * N, ROWS, HALF), BF16),
            V((2 * NB, N * CAP, HALF), BF16),
            V((2, rows, N * CAP), BF16),
            V((2, rows, 128), F32),
            V((NB, BLK), F32),
        ] + [D] * 7 + [D((N,))] * 8 + [D((NG,)), D((2 * NG,)), D((8,))],
        compiler_params=pltpu.CompilerParams(
            collective_id=0, has_side_effects=True, vmem_limit_bytes=63 * 2**20
        ),
    )(*small, gate_weight, up_weight, down_weight)


def solution(mesh):
    spread = ("dp", "expert")
    in_specs = (
        P(spread, None), P(spread, None), P(), P(), P(), P(),
        P(None, spread, None), P(None, spread, None), P(None, spread, None),
    )
    return jax.shard_map(shards, mesh=mesh, in_specs=in_specs, out_specs=P(spread, None), check_vma=False)
```

```python
import functools

import jax
import jax.numpy as jnp
import numpy as np
from jax import lax
from jax.experimental import pallas as pl
from jax.experimental.pallas import tpu as pltpu
from jax.sharding import PartitionSpec as P

MESH = pl.DeviceIdType.MESH
PIX = 4096
EPS = 1e-06
NX, NZ, NC, NY = 4, 8, 2, 4
N = NX * NZ * NC
CAP = 6
BLK = 512
NB = 8
ROWS = NB * CAP
GRP = 8
NG = N // GRP
HALF = 256
NQ = NX * NZ
LAG = 4
ROT = 20
F32, BF16 = jnp.float32, jnp.bfloat16


def place(k):
    q = lax.rem(k + ROT, NQ)
    a, m = lax.div(q, 8), lax.rem(q, 8)
    dz = lax.rem(m * 5 + 4, NZ)
    dx = lax.rem(a + 2 * m + lax.div(m, 2), NX)
    return dx, dz, lax.div(k, NQ)


def kernel(
    tok_hbm, routes_hbm, router_hbm, shift_hbm, scale_hbm, gmod_hbm, perm_hbm, weave_hbm,
    gate, up, down, out,
    tok, routes, router, shift, scale, gmod, perm, weave, WG, WD, NBUF, SB, RB, XB, H, OUT, OB, IB, ACC, PICK, SCORE, GP, DONE,
    sG, sGY, sD, sDY, sT, sO, sL, rG, rGP, rGM, rGR, rD, rDP, rDM, rDR, rT, rO, sI, sE,
):
    e = lax.axis_index("expert")
    y = lax.axis_index("dp")
    x, z, c = lax.div(e, NZ * NC), lax.rem(lax.div(e, NC), NZ), lax.rem(e, NC)
    yp, ym, y2 = lax.rem(y + 1, NY), lax.rem(y + 3, NY), lax.rem(y + 2, NY)
    above, below = (yp, e), (ym, e)

    def chip(dx, dz):
        return lax.rem(x + dx, NX) * NZ + lax.rem(z + dz, NZ)

    def tgt(k):
        dx, dz, dc = place(k)
        return chip(dx, dz) * NC + lax.rem(c + dc, NC)

    def src(k):
        dx, dz, dc = place(k)
        return chip(NX - dx, NZ - dz) * NC + lax.rem(c + dc, NC)

    def loop(lo, hi, f):
        def body(k, carry):
            f(k)
            return carry
        lax.fori_loop(lo, hi, body, 0)

    def copy(a, b, s, r, device):
        return pltpu.make_async_remote_copy(a, b, s, r, device_id=device, device_id_type=MESH)

    bar = pltpu.get_barrier_semaphore()

    def hello(k):
        b, a = lax.div(k, 8), lax.rem(k, 8)
        half = lax.div(b + 1, 2)
        dz = NZ // 2 + jnp.where(lax.rem(b, 2) == 0, half, -half)
        there = chip(NX - 1 - lax.div(a, 2), dz) * NC + lax.rem(c + 1 - lax.rem(a, 2), NC)
        pl.semaphore_signal(bar, 1, device_id=(y, there), device_id_type=MESH)

    loop(0, N - 1, hello)
    pl.semaphore_signal(bar, 1, device_id=above, device_id_type=MESH)
    pl.semaphore_signal(bar, 1, device_id=below, device_id_type=MESH)
    small = (
        (tok_hbm, tok), (routes_hbm, routes), (router_hbm, router), (shift_hbm, shift),
        (scale_hbm, scale), (gmod_hbm, gmod), (perm_hbm, perm), (weave_hbm, weave),
    )
    loads = [pltpu.make_async_copy(a, b, sI.at[i]) for i, (a, b) in enumerate(small)]
    for load in loads:
        load.start()
    pl.semaphore_wait(bar, N + 1)

    def send_g(k):
        t = tgt(k)
        copy(gate.at[t], WG.at[y * N + e, 0], sG, rG.at[k], (y, t)).start()
        copy(up.at[t], WG.at[y * N + e, 1], sG, rG.at[k], (y, t)).start()

    mine_g = WG.at[y * N + e]
    mine_d = WD.at[c * NY * NQ + y * NQ + lax.div(e, NC)]
    pltpu.make_async_copy(gate.at[e], WG.at[y * N + e, 0], sL).start()
    pltpu.make_async_copy(up.at[e], WG.at[y * N + e, 1], sL).start()
    loop(1, N, send_g)
    pltpu.make_async_copy(mine_g, mine_g, sL).wait()
    pltpu.make_async_copy(down.at[e], mine_d, sL).start()

    def send_d(k):
        t = tgt(k)
        copy(down.at[t], mine_d, sD, rD.at[k], (y, t)).start()

    loop(1, NQ, send_d)
    pltpu.make_async_copy(mine_d, mine_d, sL).wait()

    for load in loads:
        load.wait()
    count = tok.shape[0]
    image = lax.div((y * N + e) * count, PIX)
    square = jnp.zeros((count, 1), F32)
    for j in range(NB):
        v = tok[:, j * BLK:(j + 1) * BLK].astype(F32)
        square = square + jnp.sum(v * v, axis=-1, keepdims=True)
    inv = lax.rsqrt(square * (1.0 / (NB * BLK)) + EPS)
    logits = jnp.zeros((count, N), F32)
    for j in range(NB):
        cols = slice(j * BLK, (j + 1) * BLK)
        v = tok[:, cols].astype(F32)
        normed = v * inv * (1.0 + scale[pl.ds(image, 1), cols]) + shift[pl.ds(image, 1), cols]
        normed = normed.astype(BF16)
        NBUF[j] = normed
        logits = logits + lax.dot_general(
            normed, router[:, cols], (((1,), (1,)), ((), ())), preferred_element_type=F32
        )
    experts = lax.broadcasted_iota(jnp.int32, (count, N), 1)
    tall = jnp.concatenate([routes[...].astype(F32), jnp.zeros((6, count), F32)], axis=0).T
    named = [tall[:, k:k + 1].astype(jnp.int32) for k in range(2)]
    hot = [(experts == named[k]).astype(F32) for k in range(2)]
    before = (
        lax.broadcasted_iota(jnp.int32, (count, count), 1)
        < lax.broadcasted_iota(jnp.int32, (count, count), 0)
    ).astype(F32).astype(BF16)
    earlier = jnp.dot(before, (hot[0] + hot[1]).astype(BF16), preferred_element_type=F32)
    places = lax.broadcasted_iota(jnp.int32, (count, N * CAP), 1)
    near = lax.broadcasted_iota(jnp.int32, (count, ROWS), 1)
    both = None
    for k in range(2):
        r = named[k]
        ex, ez, ec = r >> 4, (r >> 1) & 7, r & 1
        dx, dz, dc = (ex - x + NX) & 3, (ez - z + NZ) & 7, (ec + c) & 1
        m = (dz * 5 + 4) & 7
        a = (dx - 2 * m - (m >> 1) + 32) & 3
        step = ((8 * a + m + NQ - ROT) & (NQ - 1)) + NQ * dc
        slot = jnp.sum(hot[k] * earlier, axis=-1, keepdims=True).astype(jnp.int32)
        spot = step * CAP + slot
        pick = (places == spot).astype(F32)
        for g in range(NG):
            PICK[g, k * count:(k + 1) * count, :] = (near == spot - g * ROWS).astype(F32).astype(BF16)
        both = pick if both is None else both + pick
        chosen = jnp.sum(hot[k] * logits, axis=-1, keepdims=True)
        SCORE[k] = jnp.broadcast_to(jax.nn.sigmoid(chosen), (count, 128))
    select = both.T.astype(BF16)

    def gather_rows(j):
        XB[j] = jnp.dot(select, NBUF[j], preferred_element_type=F32).astype(BF16)
    loop(0, NB, gather_rows)

    def clear(j):
        ACC[j] = jnp.zeros(ACC.shape[1:], F32)
    loop(0, NC * NB, clear)

    for j in range(NB):
        left = gmod[pl.ds(image, 1), j * BLK:(j + 1) * BLK]
        terms = []
        for _ in range(3):
            term = left.astype(BF16)
            terms.append(term.astype(F32))
            left = left - terms[-1]
        stack = jnp.concatenate(terms + [jnp.zeros((5, BLK), F32)], axis=0).astype(BF16)
        moved = lax.dot_general(stack, weave[...], (((1,), (1,)), ((), ())), preferred_element_type=F32)
        GP[j:j + 1] = moved[0:1] + moved[1:2] + moved[2:3]

    def rows_of(g):
        return pl.ds(pl.multiple_of(g * ROWS, 16), ROWS)

    def turn(block):
        return jnp.dot(perm[...], block, preferred_element_type=F32).astype(BF16)

    def pack(g):
        block = turn(XB[:, rows_of(g), :].reshape(NB * ROWS, BLK))
        SB[pl.ds(g * GRP, GRP)] = block.reshape(GRP, ROWS, BLK)

    def unpack(g):
        block = turn(RB[pl.ds(g * GRP, GRP)].reshape(GRP * ROWS, BLK))
        XB[:, rows_of(g), :] = block.reshape(NB, ROWS, BLK)

    def send_t(k):
        copy(SB.at[k], RB.at[k], sT, rT.at[lax.div(k, GRP)], (y, tgt(k))).start()

    def forward_g(k):
        w = WG.at[y * N + src(k)]
        copy(w, w, sGY, rGP.at[k], above).start()
        copy(w, w, sGY, rGM.at[k], below).start()

    def up_g(k):
        w = WG.at[ym * N + src(k)]
        copy(w, w, sGY, rGP.at[k], above).wait_recv()
        return w

    def down_g(k):
        w = WG.at[yp * N + src(k)]
        copy(w, w, sGY, rGM.at[k], below).wait_recv()
        return w

    def far_g(k):
        w = WG.at[y2 * N + src(k)]
        copy(w, w, sGY, rGR.at[k], above).wait_recv()

    def relay_g(k):
        def one():
            w = up_g(k)
            copy(w, w, sGY, rGR.at[k], above).start()

        def two():
            w = down_g(k)
            copy(w, w, sGY, rGR.at[k], below).start()

        lax.cond(lax.rem(k, 2) == 0, one, two)

    def last_g(k):
        def one():
            down_g(k)

        def two():
            up_g(k)

        lax.cond(lax.rem(k, 2) == 0, one, two)
        far_g(k)

    forward_g(0)

    def step_g(k):
        @pl.when(k <= NG)
        def _():
            pack(k - 1)

        @pl.when((k >= 3) & (k < NG + 3))
        def _():
            first = (k - 3) * GRP
            loop(first, first + GRP, some_t)

        @pl.when(k == NG + 3)
        def _():
            loop(NQ, N, send_d)

        w = WG.at[y * N + src(k)]
        copy(w, w, sG, rG.at[k], above).wait_recv()
        forward_g(k)

        @pl.when(k >= LAG)
        def _():
            relay_g(k - LAG)

    def some_t(k):
        @pl.when(k > 0)
        def _():
            send_t(k)

    loop(1, N, step_g)
    loop(N - LAG, N, relay_g)
    RB[0] = SB[0]

    def class_of(phase):
        return lax.rem(c + phase, NC)

    def down_at(plane, k):
        return WD.at[class_of(lax.div(k, NQ)) * NY * NQ + plane * NQ + lax.div(src(k), NC)]

    def forward_d(k):
        w = down_at(y, k)

        @pl.when(k > 0)
        def _():
            copy(w, w, sD, rD.at[k], above).wait_recv()

        copy(w, w, sDY, rDP.at[k], above).start()
        copy(w, w, sDY, rDM.at[k], below).start()

    def up_d(k):
        w = down_at(ym, k)
        copy(w, w, sDY, rDP.at[k], above).wait_recv()
        return w

    def down_d(k):
        w = down_at(yp, k)
        copy(w, w, sDY, rDM.at[k], below).wait_recv()
        return w

    def relay_d(k):
        def one():
            w = up_d(k)
            copy(w, w, sDY, rDR.at[k], above).start()

        def two():
            w = down_d(k)
            copy(w, w, sDY, rDR.at[k], below).start()

        lax.cond(lax.rem(k, 2) == 0, one, two)

    def last_d(k):
        def one():
            down_d(k)

        def two():
            up_d(k)

        lax.cond(lax.rem(k, 2) == 0, one, two)
        w = down_at(y2, k)
        copy(w, w, sDY, rDR.at[k], above).wait_recv()

    def step_d(k):
        forward_d(k)

        @pl.when(k >= LAG)
        def _():
            relay_d(k - LAG)

    def hidden(n):
        cols = pl.ds(pl.multiple_of(n * 256, 256), 256)
        g = u = None
        for j in range(NB):
            rows = slice(j * 32, (j + 1) * 32)
            a = XB[j]
            pg = jnp.dot(a, WG[rows, 0, :, cols].reshape(BLK, 256), preferred_element_type=F32)
            pu = jnp.dot(a, WG[rows, 1, :, cols].reshape(BLK, 256), preferred_element_type=F32)
            g, u = (pg, pu) if g is None else (g + pg, u + pu)
        H[:, cols] = (g / (1.0 + jnp.exp(-g)) * u).astype(BF16)

    def send_o(kind, k):
        copy(
            OB.at[kind * N + k], IB.at[kind * N + k], sO,
            rO.at[kind * NG + lax.div(k, GRP)], (y, src(k)),
        ).start()

    def multiply(phase, also):
        kind = class_of(phase)

        def block(j):
            wd = WD[pl.ds(kind * NY * NQ + j * 16, 16)].reshape(HALF, 1024)
            o = lax.dot_general(H[...], wd, (((1,), (1,)), ((), ())), preferred_element_type=F32)
            OUT[j] = o.astype(BF16)
            also(j)
        loop(0, NB, block)

    def send_back(phase, also):
        kind = class_of(phase)

        def group(g):
            block = turn(OUT[:, rows_of(g), :].reshape(NB * ROWS, HALF))
            OB[pl.ds(kind * N + g * GRP, GRP)] = block.reshape(GRP, ROWS, HALF)

            @pl.when(g > 0)
            def _():
                loop(g * GRP - GRP, g * GRP, some)

            also(g)

        def some(k):
            @pl.when(k > 0)
            def _():
                send_o(kind, k)

        loop(0, NG, group)
        loop(N - GRP, N, some)
        IB[kind * N] = OB[kind * N]

    def collect(phase):
        def group(g):
            kind = lax.rem(c + phase + lax.div(g, NG // 2), NC)

            def wait(first, size):
                there = IB.at[pl.ds(kind * N + first, size)]
                copy(there, there, sO, rO.at[kind * NG + g], above).wait_recv()

            lax.cond(g == 0, lambda: wait(1, GRP - 1), lambda: wait(g * GRP, GRP))
            block = turn(IB[pl.ds(kind * N + g * GRP, GRP)].reshape(GRP * ROWS, HALF))
            for j in range(NB):
                rows = jnp.dot(PICK[g], block[j * ROWS:(j + 1) * ROWS], preferred_element_type=F32)
                total = rows[:count] * SCORE[0][:, 0:1] + rows[count:] * SCORE[1][:, 0:1]
                ACC[kind * NB + j] = ACC[kind * NB + j] + total
        loop(0, NG, group)

    def deliver(j):
        cols = slice(j * BLK, (j + 1) * BLK)
        return pltpu.make_async_copy(DONE.at[:, cols], out.at[:, cols], sE.at[j])

    def combine(j):
        halves = [slice(kind * HALF, (kind + 1) * HALF) for kind in range(NC)]
        parts = [(GP[j:j + 1, halves[kind]] * ACC[kind * NB + j]).astype(BF16) for kind in range(NC)]
        both = jnp.concatenate(parts, axis=1)
        DONE[:, j * BLK:(j + 1) * BLK] = jnp.dot(both, weave[...], preferred_element_type=F32).astype(BF16)

    def hidden_and_pass(n):
        hidden(n)
        loop(NQ + 4 * n, NQ + 4 * n + 4, forward_d)

    def pass_more(j):
        forward_d(NQ + 16 + j)
        relay_d(NQ + j)

    def pass_most(g):
        forward_d(NQ + 24 + g)
        relay_d(NQ + 8 + g)

    def nothing(_):
        pass

    loop(0, NQ, step_d)
    loop(NQ - LAG, NQ, relay_d)
    for g in range(NG):
        there = RB.at[pl.ds(max(1, g * GRP), GRP - (g == 0))]
        copy(there, there, sT, rT.at[g], above).wait_recv()
    loop(0, NG, unpack)
    loop(0, N, last_g)
    loop(0, 4, hidden_and_pass)
    loop(0, NQ, last_d)
    multiply(0, pass_more)
    send_back(0, pass_most)
    loop(N - NQ // 2, N, relay_d)
    loop(NQ, N, last_d)
    multiply(1, nothing)
    send_back(1, nothing)
    collect(0)
    collect(1)
    for j in range(NB):
        combine(j)
        deliver(j).start()
    for j in range(NB):
        deliver(j).wait()

    def left(ref, size, s):
        view = ref.at[pl.ds(0, size)]
        copy(view, view, s, sL, above).wait_send()

    left(WG, N - 1, sG)
    left(WG, 3 * N, sGY)
    left(WD, N - 1, sD)
    left(WD, 3 * N, sDY)
    left(SB, N - 1, sT)
    left(OB, 2 * N - 2, sO)


def permutation():
    p = np.zeros((NB * ROWS, GRP * ROWS), np.float32)
    for a in range(GRP):
        for j in range(NB):
            for r in range(CAP):
                p[a * ROWS + j * CAP + r, j * ROWS + a * CAP + r] = 1.0
    return p


def weaving():
    p = np.zeros((BLK, BLK), np.float32)
    for core in range(2):
        for s in range(16):
            for i in range(16):
                p[core * HALF + s * 16 + i, s * 32 + core * 16 + i] = 1.0
    return p


def shards(tokens, routes, router_weight, shift, scale, gate_mod, gate_weight, up_weight, down_weight):
    rows, width = tokens.shape
    perm, weave = jnp.asarray(permutation(), BF16), jnp.asarray(weaving(), BF16)
    small = (tokens, routes.T, router_weight.T, shift, scale, gate_mod, perm, weave)
    D = pltpu.SemaphoreType.DMA
    V = pltpu.VMEM
    hbm = pl.BlockSpec(memory_space=pl.ANY)
    return pl.pallas_call(
        kernel,
        name="experts",
        out_shape=jax.ShapeDtypeStruct((rows, width), BF16),
        in_specs=[hbm] * 11,
        out_specs=hbm,
        scratch_shapes=[V(a.shape, a.dtype) for a in small] + [
            V((NY * N, 2, 16, 1024), BF16),
            V((NY * N, 16, 1024), BF16),
            V((NB, rows, BLK), BF16),
            V((N, ROWS, BLK), BF16),
            V((N, ROWS, BLK), BF16),
            V((NB, N * CAP, BLK), BF16),
            V((N * CAP, 1024), BF16),
            V((NB, N * CAP, HALF), BF16),
            V((2 * N, ROWS, HALF), BF16),
            V((2 * N, ROWS, HALF), BF16),
            V((2 * NB, rows, HALF), F32),
            V((NG, 2 * rows, ROWS), BF16),
            V((2, rows, 128), F32),
            V((NB, BLK), F32),
            V((rows, width), BF16),
        ] + [D] * 7 + [D((N,))] * 8 + [D((NG,)), D((2 * NG,)), D((8,)), D((NB,))],
        compiler_params=pltpu.CompilerParams(
            collective_id=0, has_side_effects=True, vmem_limit_bytes=63 * 2**20
        ),
    )(*small, gate_weight, up_weight, down_weight)


def solution(mesh):
    spread = ("dp", "expert")
    in_specs = (
        P(spread, None), P(spread, None), P(), P(), P(), P(),
        P(None, spread, None), P(None, spread, None), P(None, spread, None),
    )
    return jax.shard_map(shards, mesh=mesh, in_specs=in_specs, out_specs=P(spread, None), check_vma=False)
```

```python
import functools

import jax
import jax.numpy as jnp
import numpy as np
from jax import lax
from jax.experimental import pallas as pl
from jax.experimental.pallas import tpu as pltpu
from jax.sharding import PartitionSpec as P

MESH = pl.DeviceIdType.MESH
PIX = 4096
EPS = 1e-06
NX, NZ, NC, NY = 4, 8, 2, 4
N = NX * NZ * NC
CAP = 6
BLK = 512
NB = 8
ROWS = NB * CAP
GRP = 8
NG = N // GRP
HALF = 256
NQ = NX * NZ
LAG = 4
ROT = 20
F32, BF16 = jnp.float32, jnp.bfloat16


def place(k):
    q = lax.rem(k + ROT, NQ)
    a, m = lax.div(q, 8), lax.rem(q, 8)
    dz = lax.rem(m * 5 + 4, NZ)
    dx = lax.rem(a + 2 * m + lax.div(m, 2), NX)
    return dx, dz, lax.div(k, NQ)


def kernel(
    tok_hbm, routes_hbm, router_hbm, shift_hbm, scale_hbm, gmod_hbm, perm_hbm, weave_hbm,
    gate, up, down, out,
    tok, routes, router, shift, scale, gmod, perm, weave, WG, WD, NBUF, SB, RB, XB, H, OUT, OB, IB, ACC, PICK, SCORE, GP, DONE,
    sG, sGY, sD, sDY, sT, sO, sL, rG, rGY, rD, rDY, rT, rO, sI, sE,
):
    e = lax.axis_index("expert")
    y = lax.axis_index("dp")
    x, z, c = lax.div(e, NZ * NC), lax.rem(lax.div(e, NC), NZ), lax.rem(e, NC)
    yp, ym, y2 = lax.rem(y + 1, NY), lax.rem(y + 3, NY), lax.rem(y + 2, NY)
    above, below = (yp, e), (ym, e)

    def chip(dx, dz):
        return lax.rem(x + dx, NX) * NZ + lax.rem(z + dz, NZ)

    def tgt(k):
        dx, dz, dc = place(k)
        return chip(dx, dz) * NC + lax.rem(c + dc, NC)

    def src(k):
        dx, dz, dc = place(k)
        return chip(NX - dx, NZ - dz) * NC + lax.rem(c + dc, NC)

    def loop(lo, hi, f):
        def body(k, carry):
            f(k)
            return carry
        lax.fori_loop(lo, hi, body, 0)

    def copy(a, b, s, r, device):
        return pltpu.make_async_remote_copy(a, b, s, r, device_id=device, device_id_type=MESH)

    bar = pltpu.get_barrier_semaphore()

    def hello(k):
        b, a = lax.div(k, 8), lax.rem(k, 8)
        half = lax.div(b + 1, 2)
        dz = NZ // 2 + jnp.where(lax.rem(b, 2) == 0, half, -half)
        there = chip(NX - 1 - lax.div(a, 2), dz) * NC + lax.rem(c + 1 - lax.rem(a, 2), NC)
        pl.semaphore_signal(bar, 1, device_id=(y, there), device_id_type=MESH)

    loop(0, N - 1, hello)
    pl.semaphore_signal(bar, 1, device_id=above, device_id_type=MESH)
    pl.semaphore_signal(bar, 1, device_id=below, device_id_type=MESH)
    small = (
        (tok_hbm, tok), (routes_hbm, routes), (router_hbm, router), (shift_hbm, shift),
        (scale_hbm, scale), (gmod_hbm, gmod), (perm_hbm, perm), (weave_hbm, weave),
    )
    loads = [pltpu.make_async_copy(a, b, sI.at[i]) for i, (a, b) in enumerate(small)]
    for load in loads:
        load.start()
    pl.semaphore_wait(bar, N + 1)

    def send_g(k):
        t = tgt(k)
        copy(gate.at[t], WG.at[y * N + e, 0], sG, rG.at[k], (y, t)).start()
        copy(up.at[t], WG.at[y * N + e, 1], sG, rG.at[k], (y, t)).start()

    mine_g = WG.at[y * N + e]
    mine_d = WD.at[c * NY * NQ + y * NQ + lax.div(e, NC)]
    pltpu.make_async_copy(gate.at[e], WG.at[y * N + e, 0], sL).start()
    pltpu.make_async_copy(up.at[e], WG.at[y * N + e, 1], sL).start()
    loop(1, N, send_g)
    pltpu.make_async_copy(mine_g, mine_g, sL).wait()
    pltpu.make_async_copy(down.at[e], mine_d, sL).start()

    def send_d(k):
        t = tgt(k)
        copy(down.at[t], mine_d, sD, rD.at[k], (y, t)).start()

    loop(1, NQ, send_d)
    pltpu.make_async_copy(mine_d, mine_d, sL).wait()

    for load in loads:
        load.wait()
    count = tok.shape[0]
    image = lax.div((y * N + e) * count, PIX)
    square = jnp.zeros((count, 1), F32)
    for j in range(NB):
        v = tok[:, j * BLK:(j + 1) * BLK].astype(F32)
        square = square + jnp.sum(v * v, axis=-1, keepdims=True)
    inv = lax.rsqrt(square * (1.0 / (NB * BLK)) + EPS)
    logits = jnp.zeros((count, N), F32)
    for j in range(NB):
        cols = slice(j * BLK, (j + 1) * BLK)
        v = tok[:, cols].astype(F32)
        normed = v * inv * (1.0 + scale[pl.ds(image, 1), cols]) + shift[pl.ds(image, 1), cols]
        normed = normed.astype(BF16)
        NBUF[j] = normed
        logits = logits + lax.dot_general(
            normed, router[:, cols], (((1,), (1,)), ((), ())), preferred_element_type=F32
        )
    experts = lax.broadcasted_iota(jnp.int32, (count, N), 1)
    tall = jnp.concatenate([routes[...].astype(F32), jnp.zeros((6, count), F32)], axis=0).T
    named = [tall[:, k:k + 1].astype(jnp.int32) for k in range(2)]
    hot = [(experts == named[k]).astype(F32) for k in range(2)]
    before = (
        lax.broadcasted_iota(jnp.int32, (count, count), 1)
        < lax.broadcasted_iota(jnp.int32, (count, count), 0)
    ).astype(F32).astype(BF16)
    earlier = jnp.dot(before, (hot[0] + hot[1]).astype(BF16), preferred_element_type=F32)
    places = lax.broadcasted_iota(jnp.int32, (count, N * CAP), 1)
    near = lax.broadcasted_iota(jnp.int32, (count, ROWS), 1)
    both = None
    for k in range(2):
        r = named[k]
        ex, ez, ec = r >> 4, (r >> 1) & 7, r & 1
        dx, dz, dc = (ex - x + NX) & 3, (ez - z + NZ) & 7, (ec + c) & 1
        m = (dz * 5 + 4) & 7
        a = (dx - 2 * m - (m >> 1) + 32) & 3
        step = ((8 * a + m + NQ - ROT) & (NQ - 1)) + NQ * dc
        slot = jnp.sum(hot[k] * earlier, axis=-1, keepdims=True).astype(jnp.int32)
        spot = step * CAP + slot
        pick = (places == spot).astype(F32)
        for g in range(NG):
            PICK[g, k * count:(k + 1) * count, :] = (near == spot - g * ROWS).astype(F32).astype(BF16)
        both = pick if both is None else both + pick
        chosen = jnp.sum(hot[k] * logits, axis=-1, keepdims=True)
        SCORE[k] = jnp.broadcast_to(jax.nn.sigmoid(chosen), (count, 128))
    select = both.T.astype(BF16)

    def gather_rows(j):
        XB[j] = jnp.dot(select, NBUF[j], preferred_element_type=F32).astype(BF16)
    loop(0, NB, gather_rows)

    def clear(j):
        ACC[j] = jnp.zeros(ACC.shape[1:], F32)
    loop(0, NC * NB, clear)

    for j in range(NB):
        left = gmod[pl.ds(image, 1), j * BLK:(j + 1) * BLK]
        terms = []
        for _ in range(3):
            term = left.astype(BF16)
            terms.append(term.astype(F32))
            left = left - terms[-1]
        stack = jnp.concatenate(terms + [jnp.zeros((5, BLK), F32)], axis=0).astype(BF16)
        for q in range(2):
            moved = lax.dot_general(
                stack[:, q * HALF:(q + 1) * HALF], weave[...], (((1,), (1,)), ((), ())),
                preferred_element_type=F32,
            )
            moved = moved[0:1] + moved[1:2] + moved[2:3]
            for kind in range(NC):
                at = kind * HALF + q * 128
                GP[j:j + 1, at:at + 128] = moved[:, kind * 128:(kind + 1) * 128]

    def rows_of(g):
        return pl.ds(pl.multiple_of(g * ROWS, 16), ROWS)

    def turn(block):
        return jnp.dot(perm[...], block, preferred_element_type=F32).astype(BF16)

    def pack(g):
        block = turn(XB[:, rows_of(g), :].reshape(NB * ROWS, BLK))
        SB[pl.ds(g * GRP, GRP)] = block.reshape(GRP, ROWS, BLK)

    def unpack(g):
        block = turn(RB[pl.ds(g * GRP, GRP)].reshape(GRP * ROWS, BLK))
        XB[:, rows_of(g), :] = block.reshape(NB, ROWS, BLK)

    def send_t(k):
        copy(SB.at[k], RB.at[k], sT, rT.at[lax.div(k, GRP)], (y, tgt(k))).start()

    def above_slot(k, shared):
        return k + lax.rem(k, 2) * (shared + 1 - k)

    def below_slot(k, shared):
        return shared + lax.rem(k, 2) * (k - shared)

    def forward_g(k):
        w = WG.at[y * N + src(k)]
        copy(w, w, sGY, rGY.at[above_slot(k, N)], above).start()
        copy(w, w, sGY, rGY.at[below_slot(k, N)], below).start()

    def relay_g(k):
        def one():
            w = WG.at[ym * N + src(k)]
            copy(w, w, sGY, rGY.at[k], above).wait_recv()
            copy(w, w, sGY, rGY.at[N + 2], above).start()

        def two():
            w = WG.at[yp * N + src(k)]
            copy(w, w, sGY, rGY.at[k], below).wait_recv()
            copy(w, w, sGY, rGY.at[N + 2], below).start()

        lax.cond(lax.rem(k, 2) == 0, one, two)

    def arrived(ref, first, size, s):
        w = ref.at[pl.ds(first, size)]
        copy(w, w, sL, s, above).wait_recv()

    def last_g():
        arrived(WG, yp * N, N // 2, rGY.at[N])
        arrived(WG, ym * N, N // 2, rGY.at[N + 1])
        arrived(WG, y2 * N, N, rGY.at[N + 2])

    forward_g(0)

    def step_g(k):
        @pl.when(k <= NG)
        def _():
            pack(k - 1)

        @pl.when((k >= 3) & (k < NG + 3))
        def _():
            first = (k - 3) * GRP
            loop(first, first + GRP, some_t)

        @pl.when(k == NG + 3)
        def _():
            loop(NQ, N, send_d)

        w = WG.at[y * N + src(k)]
        copy(w, w, sG, rG.at[k], above).wait_recv()
        forward_g(k)

        @pl.when(k >= LAG)
        def _():
            relay_g(k - LAG)

    def some_t(k):
        @pl.when(k > 0)
        def _():
            send_t(k)

    loop(1, N, step_g)
    loop(N - LAG, N, relay_g)
    RB[0] = SB[0]

    def class_of(phase):
        return lax.rem(c + phase, NC)

    def down_at(plane, k):
        return WD.at[class_of(lax.div(k, NQ)) * NY * NQ + plane * NQ + lax.div(src(k), NC)]

    def forward_d(k):
        w = down_at(y, k)

        @pl.when(k > 0)
        def _():
            copy(w, w, sD, rD.at[k], above).wait_recv()

        shared = N + 3 * lax.div(k, NQ)
        copy(w, w, sDY, rDY.at[above_slot(k, shared)], above).start()
        copy(w, w, sDY, rDY.at[below_slot(k, shared)], below).start()

    def relay_d(k):
        shared = N + 3 * lax.div(k, NQ)

        def one():
            w = down_at(ym, k)
            copy(w, w, sDY, rDY.at[k], above).wait_recv()
            copy(w, w, sDY, rDY.at[shared + 2], above).start()

        def two():
            w = down_at(yp, k)
            copy(w, w, sDY, rDY.at[k], below).wait_recv()
            copy(w, w, sDY, rDY.at[shared + 2], below).start()

        lax.cond(lax.rem(k, 2) == 0, one, two)

    def last_d(phase):
        first, shared = class_of(phase) * NY * NQ, N + 3 * phase
        arrived(WD, first + yp * NQ, NQ // 2, rDY.at[shared])
        arrived(WD, first + ym * NQ, NQ // 2, rDY.at[shared + 1])
        arrived(WD, first + y2 * NQ, NQ, rDY.at[shared + 2])

    def step_d(k):
        forward_d(k)

        @pl.when(k >= LAG)
        def _():
            relay_d(k - LAG)

    def hidden(n):
        cols = pl.ds(pl.multiple_of(n * 256, 256), 256)
        g = u = None
        for j in range(NB):
            rows = slice(j * 32, (j + 1) * 32)
            a = XB[j]
            pg = jnp.dot(a, WG[rows, 0, :, cols].reshape(BLK, 256), preferred_element_type=F32)
            pu = jnp.dot(a, WG[rows, 1, :, cols].reshape(BLK, 256), preferred_element_type=F32)
            g, u = (pg, pu) if g is None else (g + pg, u + pu)
        H[:, cols] = (g / (1.0 + jnp.exp(-g)) * u).astype(BF16)

    def send_o(kind, k):
        copy(
            OB.at[kind * N + k], IB.at[kind * N + k], sO,
            rO.at[kind * NG + lax.div(k, GRP)], (y, src(k)),
        ).start()

    def multiply(phase, also):
        kind = class_of(phase)

        def block(j):
            wd = WD[pl.ds(kind * NY * NQ + j * 16, 16)].reshape(HALF, 1024)
            o = lax.dot_general(H[...], wd, (((1,), (1,)), ((), ())), preferred_element_type=F32)
            OUT[j] = o.astype(BF16)
            also(j)
        loop(0, NB, block)

    def send_back(phase, also):
        kind = class_of(phase)

        def group(g):
            block = turn(OUT[:, rows_of(g), :].reshape(NB * ROWS, HALF))
            OB[pl.ds(kind * N + g * GRP, GRP)] = block.reshape(GRP, ROWS, HALF)

            @pl.when(g > 0)
            def _():
                loop(g * GRP - GRP, g * GRP, some)

            also(g)

        def some(k):
            @pl.when(k > 0)
            def _():
                send_o(kind, k)

        loop(0, NG, group)
        loop(N - GRP, N, some)
        IB[kind * N] = OB[kind * N]

    def collect(phase):
        def group(g):
            kind = lax.rem(c + phase + lax.div(g, NG // 2), NC)

            def wait(first, size):
                there = IB.at[pl.ds(kind * N + first, size)]
                copy(there, there, sO, rO.at[kind * NG + g], above).wait_recv()

            lax.cond(g == 0, lambda: wait(1, GRP - 1), lambda: wait(g * GRP, GRP))
            block = turn(IB[pl.ds(kind * N + g * GRP, GRP)].reshape(GRP * ROWS, HALF))
            for j in range(NB):
                rows = jnp.dot(PICK[g], block[j * ROWS:(j + 1) * ROWS], preferred_element_type=F32)
                total = rows[:count] * SCORE[0][:, 0:1] + rows[count:] * SCORE[1][:, 0:1]
                ACC[kind * NB + j] = ACC[kind * NB + j] + total
        loop(0, NG, group)

    def deliver(j):
        cols = slice(j * BLK, (j + 1) * BLK)
        return pltpu.make_async_copy(DONE.at[:, cols], out.at[:, cols], sE.at[j])

    def combine(some):
        stack = []
        for j in some:
            halves = [slice(kind * HALF, (kind + 1) * HALF) for kind in range(NC)]
            parts = [(GP[j:j + 1, halves[kind]] * ACC[kind * NB + j]).astype(BF16) for kind in range(NC)]
            for q in range(2):
                stack.append(jnp.concatenate([part[:, q * 128:(q + 1) * 128] for part in parts], axis=1))
        rows = jnp.dot(jnp.concatenate(stack, axis=0), weave[...], preferred_element_type=F32).astype(BF16)
        for i, j in enumerate(some):
            for q in range(2):
                at, row = j * BLK + q * HALF, (2 * i + q) * count
                DONE[:, at:at + HALF] = rows[row:row + count]

    def hidden_and_pass(n):
        hidden(n)
        loop(NQ + 4 * n, NQ + 4 * n + 4, forward_d)

    def pass_more(j):
        forward_d(NQ + 16 + j)
        relay_d(NQ + j)

    def pass_most(g):
        forward_d(NQ + 24 + g)
        relay_d(NQ + 8 + g)

    def nothing(_):
        pass

    loop(0, NQ, step_d)
    loop(NQ - LAG, NQ, relay_d)
    for g in range(NG):
        there = RB.at[pl.ds(max(1, g * GRP), GRP - (g == 0))]
        copy(there, there, sT, rT.at[g], above).wait_recv()
    loop(0, NG, unpack)
    last_g()
    loop(0, 4, hidden_and_pass)
    last_d(0)
    multiply(0, pass_more)
    send_back(0, pass_most)
    loop(N - NQ // 2, N, relay_d)
    last_d(1)
    multiply(1, nothing)
    send_back(1, nothing)
    collect(0)
    collect(1)
    for j in range(0, NB, 2):
        combine((j, j + 1))
        deliver(j).start()
        deliver(j + 1).start()
    for j in range(NB):
        deliver(j).wait()

    def left(ref, size, s):
        view = ref.at[pl.ds(0, size)]
        copy(view, view, s, sL, above).wait_send()

    left(WG, N - 1, sG)
    left(WG, 3 * N, sGY)
    left(WD, N - 1, sD)
    left(WD, 3 * N, sDY)
    left(SB, N - 1, sT)
    left(OB, 2 * N - 2, sO)


def permutation():
    p = np.zeros((NB * ROWS, GRP * ROWS), np.float32)
    for a in range(GRP):
        for j in range(NB):
            for r in range(CAP):
                p[a * ROWS + j * CAP + r, j * ROWS + a * CAP + r] = 1.0
    return p


def weaving():
    p = np.zeros((HALF, HALF), np.float32)
    for core in range(2):
        for s in range(8):
            for i in range(16):
                p[core * 128 + s * 16 + i, s * 32 + core * 16 + i] = 1.0
    return p


def shards(tokens, routes, router_weight, shift, scale, gate_mod, gate_weight, up_weight, down_weight):
    rows, width = tokens.shape
    perm, weave = jnp.asarray(permutation(), BF16), jnp.asarray(weaving(), BF16)
    small = (tokens, routes.T, router_weight.T, shift, scale, gate_mod, perm, weave)
    D = pltpu.SemaphoreType.DMA
    V = pltpu.VMEM
    hbm = pl.BlockSpec(memory_space=pl.ANY)
    return pl.pallas_call(
        kernel,
        name="experts",
        out_shape=jax.ShapeDtypeStruct((rows, width), BF16),
        in_specs=[hbm] * 11,
        out_specs=hbm,
        scratch_shapes=[V(a.shape, a.dtype) for a in small] + [
            V((NY * N, 2, 16, 1024), BF16),
            V((NY * N, 16, 1024), BF16),
            V((NB, rows, BLK), BF16),
            V((N, ROWS, BLK), BF16),
            V((N, ROWS, BLK), BF16),
            V((NB, N * CAP, BLK), BF16),
            V((N * CAP, 1024), BF16),
            V((NB, N * CAP, HALF), BF16),
            V((2 * N, ROWS, HALF), BF16),
            V((2 * N, ROWS, HALF), BF16),
            V((2 * NB, rows, HALF), F32),
            V((NG, 2 * rows, ROWS), BF16),
            V((2, rows, 128), F32),
            V((NB, BLK), F32),
            V((rows, width), BF16),
        ] + [D] * 7 + [D((N,)), D((N + 3,)), D((N,)), D((N + 6,))] + [D((NG,)), D((2 * NG,)), D((8,)), D((NB,))],
        compiler_params=pltpu.CompilerParams(
            collective_id=0, has_side_effects=True, vmem_limit_bytes=63 * 2**20
        ),
    )(*small, gate_weight, up_weight, down_weight)


def solution(mesh):
    spread = ("dp", "expert")
    in_specs = (
        P(spread, None), P(spread, None), P(), P(), P(), P(),
        P(None, spread, None), P(None, spread, None), P(None, spread, None),
    )
    return jax.shard_map(shards, mesh=mesh, in_specs=in_specs, out_specs=P(spread, None), check_vma=False)
```

```python
import functools

import jax
import jax.numpy as jnp
import numpy as np
from jax import lax
from jax.experimental import pallas as pl
from jax.experimental.pallas import tpu as pltpu
from jax.sharding import PartitionSpec as P

MESH = pl.DeviceIdType.MESH
PIX = 4096
EPS = 1e-06
NX, NZ, NC, NY = 4, 8, 2, 4
N = NX * NZ * NC
CAP = 6
BLK = 512
NB = 8
ROWS = NB * CAP
GRP = 8
NG = N // GRP
HALF = 256
NQ = NX * NZ
LAG = 4
ROT = 20
F32, BF16 = jnp.float32, jnp.bfloat16


def place(k):
    q = lax.rem(k + ROT, NQ)
    a, m = lax.div(q, 8), lax.rem(q, 8)
    dz = lax.rem(m * 7 + 4, NZ)
    dx = lax.rem(a + 2 * m + lax.div(m, 2), NX)
    return dx, dz, lax.div(k, NQ)


def kernel(
    tok_hbm, routes_hbm, router_hbm, shift_hbm, scale_hbm, gmod_hbm, perm_hbm, weave_hbm,
    gate, up, down, out,
    tok, routes, router, shift, scale, gmod, perm, weave, WG, WD, NBUF, SB, RB, XB, H, OUT, OB, IB, ACC, PICK, SCORE, GP, DONE,
    sG, sGY, sD, sDY, sT, sO, sL, rG, rGY, rD, rDY, rT, rO, sI, sE,
):
    e = lax.axis_index("expert")
    y = lax.axis_index("dp")
    x, z, c = lax.div(e, NZ * NC), lax.rem(lax.div(e, NC), NZ), lax.rem(e, NC)
    yp, ym, y2 = lax.rem(y + 1, NY), lax.rem(y + 3, NY), lax.rem(y + 2, NY)
    above, below = (yp, e), (ym, e)

    def chip(dx, dz):
        return lax.rem(x + dx, NX) * NZ + lax.rem(z + dz, NZ)

    def tgt(k):
        dx, dz, dc = place(k)
        return chip(dx, dz) * NC + lax.rem(c + dc, NC)

    def src(k):
        dx, dz, dc = place(k)
        return chip(NX - dx, NZ - dz) * NC + lax.rem(c + dc, NC)

    def loop(lo, hi, f):
        def body(k, carry):
            f(k)
            return carry
        lax.fori_loop(lo, hi, body, 0)

    def copy(a, b, s, r, device):
        return pltpu.make_async_remote_copy(a, b, s, r, device_id=device, device_id_type=MESH)

    bar = pltpu.get_barrier_semaphore()

    along_x = [lax.rem(x + d, NX) * (NZ * NC) for d in range(NX)]
    along_z = [lax.rem(z + d, NZ) * NC for d in range(NZ)]
    along_c = [lax.rem(c + d, NC) for d in range(NC)]
    for dz in (4, 3, 5, 2, 6, 1, 7, 0):
        for dx in (2, 1, 3, 0):
            for dc in range(NC):
                if dz or dx or dc:
                    there = along_x[dx] + along_z[dz] + along_c[dc]
                    pl.semaphore_signal(bar, 1, device_id=(y, there), device_id_type=MESH)
    pl.semaphore_signal(bar, 1, device_id=above, device_id_type=MESH)
    pl.semaphore_signal(bar, 1, device_id=below, device_id_type=MESH)
    small = (
        (tok_hbm, tok), (routes_hbm, routes), (router_hbm, router), (shift_hbm, shift),
        (scale_hbm, scale), (gmod_hbm, gmod), (perm_hbm, perm), (weave_hbm, weave),
    )
    loads = [pltpu.make_async_copy(a, b, sI.at[i]) for i, (a, b) in enumerate(small)]
    for load in loads:
        load.start()
    pl.semaphore_wait(bar, N + 1)

    def send_g(k):
        t = tgt(k)
        copy(gate.at[t], WG.at[y * N + e, 0], sG, rG.at[k], (y, t)).start()
        copy(up.at[t], WG.at[y * N + e, 1], sG, rG.at[k], (y, t)).start()

    mine_g = WG.at[y * N + e]
    mine_d = WD.at[c * NY * NQ + y * NQ + lax.div(e, NC)]
    pltpu.make_async_copy(gate.at[e], WG.at[y * N + e, 0], sL).start()
    pltpu.make_async_copy(up.at[e], WG.at[y * N + e, 1], sL).start()
    loop(1, N, send_g)
    pltpu.make_async_copy(mine_g, mine_g, sL).wait()
    pltpu.make_async_copy(down.at[e], mine_d, sL).start()

    def send_d(k):
        t = tgt(k)
        copy(down.at[t], mine_d, sD, rD.at[k], (y, t)).start()

    loop(1, NQ, send_d)
    pltpu.make_async_copy(mine_d, mine_d, sL).wait()

    for load in loads:
        load.wait()
    count = tok.shape[0]
    image = lax.div((y * N + e) * count, PIX)
    square = jnp.zeros((count, 1), F32)
    for j in range(NB):
        v = tok[:, j * BLK:(j + 1) * BLK].astype(F32)
        square = square + jnp.sum(v * v, axis=-1, keepdims=True)
    inv = lax.rsqrt(square * (1.0 / (NB * BLK)) + EPS)
    logits = jnp.zeros((count, N), F32)
    for j in range(NB):
        cols = slice(j * BLK, (j + 1) * BLK)
        v = tok[:, cols].astype(F32)
        normed = v * inv * (1.0 + scale[pl.ds(image, 1), cols]) + shift[pl.ds(image, 1), cols]
        normed = normed.astype(BF16)
        NBUF[j] = normed
        logits = logits + lax.dot_general(
            normed, router[:, cols], (((1,), (1,)), ((), ())), preferred_element_type=F32
        )
    experts = lax.broadcasted_iota(jnp.int32, (count, N), 1)
    tall = jnp.concatenate([routes[...].astype(F32), jnp.zeros((6, count), F32)], axis=0).T
    named = [tall[:, k:k + 1].astype(jnp.int32) for k in range(2)]
    hot = [(experts == named[k]).astype(F32) for k in range(2)]
    before = (
        lax.broadcasted_iota(jnp.int32, (count, count), 1)
        < lax.broadcasted_iota(jnp.int32, (count, count), 0)
    ).astype(F32).astype(BF16)
    earlier = jnp.dot(before, (hot[0] + hot[1]).astype(BF16), preferred_element_type=F32)
    places = lax.broadcasted_iota(jnp.int32, (count, N * CAP), 1)
    near = lax.broadcasted_iota(jnp.int32, (count, ROWS), 1)
    both = None
    for k in range(2):
        r = named[k]
        ex, ez, ec = r >> 4, (r >> 1) & 7, r & 1
        dx, dz, dc = (ex - x + NX) & 3, (ez - z + NZ) & 7, (ec + c) & 1
        m = (dz * 7 + 4) & 7
        a = (dx - 2 * m - (m >> 1) + 32) & 3
        step = ((8 * a + m + NQ - ROT) & (NQ - 1)) + NQ * dc
        slot = jnp.sum(hot[k] * earlier, axis=-1, keepdims=True).astype(jnp.int32)
        spot = step * CAP + slot
        pick = (places == spot).astype(F32)
        for g in range(NG):
            PICK[g, k * count:(k + 1) * count, :] = (near == spot - g * ROWS).astype(F32).astype(BF16)
        both = pick if both is None else both + pick
        chosen = jnp.sum(hot[k] * logits, axis=-1, keepdims=True)
        SCORE[k] = jnp.broadcast_to(jax.nn.sigmoid(chosen), (count, 128))
    select = both.T.astype(BF16)

    def gather_rows(j):
        XB[j] = jnp.dot(select, NBUF[j], preferred_element_type=F32).astype(BF16)
    loop(0, NB, gather_rows)

    def clear(j):
        ACC[j] = jnp.zeros(ACC.shape[1:], F32)
    loop(0, NC * NB, clear)

    for j in range(NB):
        left = gmod[pl.ds(image, 1), j * BLK:(j + 1) * BLK]
        terms = []
        for _ in range(3):
            term = left.astype(BF16)
            terms.append(term.astype(F32))
            left = left - terms[-1]
        stack = jnp.concatenate(terms + [jnp.zeros((5, BLK), F32)], axis=0).astype(BF16)
        for q in range(2):
            moved = lax.dot_general(
                stack[:, q * HALF:(q + 1) * HALF], weave[...], (((1,), (1,)), ((), ())),
                preferred_element_type=F32,
            )
            moved = moved[0:1] + moved[1:2] + moved[2:3]
            for kind in range(NC):
                at = kind * HALF + q * 128
                GP[j:j + 1, at:at + 128] = moved[:, kind * 128:(kind + 1) * 128]

    def rows_of(g):
        return pl.ds(pl.multiple_of(g * ROWS, 16), ROWS)

    def turn(block):
        return jnp.dot(perm[...], block, preferred_element_type=F32).astype(BF16)

    def pack(g):
        block = turn(XB[:, rows_of(g), :].reshape(NB * ROWS, BLK))
        SB[pl.ds(g * GRP, GRP)] = block.reshape(GRP, ROWS, BLK)

    def unpack(g):
        block = turn(RB[pl.ds(g * GRP, GRP)].reshape(GRP * ROWS, BLK))
        XB[:, rows_of(g), :] = block.reshape(NB, ROWS, BLK)

    def send_t(k):
        copy(SB.at[k], RB.at[k], sT, rT.at[lax.div(k, GRP)], (y, tgt(k))).start()

    def above_slot(k, shared):
        return k + lax.rem(k, 2) * (shared + 1 - k)

    def below_slot(k, shared):
        return shared + lax.rem(k, 2) * (k - shared)

    def forward_g(k):
        w = WG.at[y * N + src(k)]
        copy(w, w, sGY, rGY.at[above_slot(k, N)], above).start()
        copy(w, w, sGY, rGY.at[below_slot(k, N)], below).start()

    def relay_g(k):
        def one():
            w = WG.at[ym * N + src(k)]
            copy(w, w, sGY, rGY.at[k], above).wait_recv()
            copy(w, w, sGY, rGY.at[N + 2], above).start()

        def two():
            w = WG.at[yp * N + src(k)]
            copy(w, w, sGY, rGY.at[k], below).wait_recv()
            copy(w, w, sGY, rGY.at[N + 2], below).start()

        lax.cond(lax.rem(k, 2) == 0, one, two)

    def arrived(ref, first, size, s):
        w = ref.at[pl.ds(first, size)]
        copy(w, w, sL, s, above).wait_recv()

    def last_g():
        arrived(WG, yp * N, N // 2, rGY.at[N])
        arrived(WG, ym * N, N // 2, rGY.at[N + 1])
        arrived(WG, y2 * N, N, rGY.at[N + 2])

    forward_g(0)

    def step_g(k):
        @pl.when(k <= NG)
        def _():
            pack(k - 1)

        @pl.when((k >= 3) & (k < NG + 3))
        def _():
            first = (k - 3) * GRP
            loop(first, first + GRP, some_t)

        @pl.when(k == NG + 3)
        def _():
            loop(NQ, N, send_d)

        w = WG.at[y * N + src(k)]
        copy(w, w, sG, rG.at[k], above).wait_recv()
        forward_g(k)

        @pl.when(k >= LAG)
        def _():
            relay_g(k - LAG)

    def some_t(k):
        @pl.when(k > 0)
        def _():
            send_t(k)

    loop(1, N, step_g)
    loop(N - LAG, N, relay_g)
    RB[0] = SB[0]

    def class_of(phase):
        return lax.rem(c + phase, NC)

    def down_at(plane, k):
        return WD.at[class_of(lax.div(k, NQ)) * NY * NQ + plane * NQ + lax.div(src(k), NC)]

    def forward_d(k):
        w = down_at(y, k)

        @pl.when(k > 0)
        def _():
            copy(w, w, sD, rD.at[k], above).wait_recv()

        shared = N + 3 * lax.div(k, NQ)
        copy(w, w, sDY, rDY.at[above_slot(k, shared)], above).start()
        copy(w, w, sDY, rDY.at[below_slot(k, shared)], below).start()

    def relay_d(k):
        shared = N + 3 * lax.div(k, NQ)

        def one():
            w = down_at(ym, k)
            copy(w, w, sDY, rDY.at[k], above).wait_recv()
            copy(w, w, sDY, rDY.at[shared + 2], above).start()

        def two():
            w = down_at(yp, k)
            copy(w, w, sDY, rDY.at[k], below).wait_recv()
            copy(w, w, sDY, rDY.at[shared + 2], below).start()

        lax.cond(lax.rem(k, 2) == 0, one, two)

    def last_d(phase):
        first, shared = class_of(phase) * NY * NQ, N + 3 * phase
        arrived(WD, first + yp * NQ, NQ // 2, rDY.at[shared])
        arrived(WD, first + ym * NQ, NQ // 2, rDY.at[shared + 1])
        arrived(WD, first + y2 * NQ, NQ, rDY.at[shared + 2])

    def step_d(k):
        forward_d(k)

        @pl.when(k >= LAG)
        def _():
            relay_d(k - LAG)

    def hidden(n):
        cols = pl.ds(pl.multiple_of(n * 256, 256), 256)
        g = u = None
        for j in range(NB):
            rows = slice(j * 32, (j + 1) * 32)
            a = XB[j]
            pg = jnp.dot(a, WG[rows, 0, :, cols].reshape(BLK, 256), preferred_element_type=F32)
            pu = jnp.dot(a, WG[rows, 1, :, cols].reshape(BLK, 256), preferred_element_type=F32)
            g, u = (pg, pu) if g is None else (g + pg, u + pu)
        H[:, cols] = (g / (1.0 + jnp.exp(-g)) * u).astype(BF16)

    def send_o(kind, k):
        copy(
            OB.at[kind * N + k], IB.at[kind * N + k], sO,
            rO.at[kind * NG + lax.div(k, GRP)], (y, src(k)),
        ).start()

    def multiply(phase, also):
        kind = class_of(phase)

        def block(j):
            wd = WD[pl.ds(kind * NY * NQ + j * 16, 16)].reshape(HALF, 1024)
            o = lax.dot_general(H[...], wd, (((1,), (1,)), ((), ())), preferred_element_type=F32)
            OUT[j] = o.astype(BF16)
            also(j)
        loop(0, NB, block)

    def send_back(phase, also):
        kind = class_of(phase)

        def group(g):
            block = turn(OUT[:, rows_of(g), :].reshape(NB * ROWS, HALF))
            OB[pl.ds(kind * N + g * GRP, GRP)] = block.reshape(GRP, ROWS, HALF)

            @pl.when(g > 0)
            def _():
                loop(g * GRP - GRP, g * GRP, some)

            also(g)

        def some(k):
            @pl.when(k > 0)
            def _():
                send_o(kind, k)

        loop(0, NG, group)
        loop(N - GRP, N, some)
        IB[kind * N] = OB[kind * N]

    def collect(phase):
        def group(g):
            kind = lax.rem(c + phase + lax.div(g, NG // 2), NC)

            def wait(first, size):
                there = IB.at[pl.ds(kind * N + first, size)]
                copy(there, there, sO, rO.at[kind * NG + g], above).wait_recv()

            lax.cond(g == 0, lambda: wait(1, GRP - 1), lambda: wait(g * GRP, GRP))
            block = turn(IB[pl.ds(kind * N + g * GRP, GRP)].reshape(GRP * ROWS, HALF))
            for j in range(NB):
                rows = jnp.dot(PICK[g], block[j * ROWS:(j + 1) * ROWS], preferred_element_type=F32)
                total = rows[:count] * SCORE[0][:, 0:1] + rows[count:] * SCORE[1][:, 0:1]
                ACC[kind * NB + j] = ACC[kind * NB + j] + total
        loop(0, NG, group)

    def deliver(j):
        cols = slice(j * BLK, (j + 1) * BLK)
        return pltpu.make_async_copy(DONE.at[:, cols], out.at[:, cols], sE.at[j])

    def combine(some):
        stack = []
        for j in some:
            halves = [slice(kind * HALF, (kind + 1) * HALF) for kind in range(NC)]
            parts = [(GP[j:j + 1, halves[kind]] * ACC[kind * NB + j]).astype(BF16) for kind in range(NC)]
            for q in range(2):
                stack.append(jnp.concatenate([part[:, q * 128:(q + 1) * 128] for part in parts], axis=1))
        rows = jnp.dot(jnp.concatenate(stack, axis=0), weave[...], preferred_element_type=F32).astype(BF16)
        for i, j in enumerate(some):
            for q in range(2):
                at, row = j * BLK + q * HALF, (2 * i + q) * count
                DONE[:, at:at + HALF] = rows[row:row + count]

    def hidden_and_pass(n):
        hidden(n)
        loop(NQ + 4 * n, NQ + 4 * n + 4, forward_d)

    def pass_more(j):
        forward_d(NQ + 16 + j)
        relay_d(NQ + j)

    def pass_most(g):
        forward_d(NQ + 24 + g)
        relay_d(NQ + 8 + g)

    def nothing(_):
        pass

    loop(0, NQ, step_d)
    loop(NQ - LAG, NQ, relay_d)
    for g in range(NG):
        there = RB.at[pl.ds(max(1, g * GRP), GRP - (g == 0))]
        copy(there, there, sT, rT.at[g], above).wait_recv()
    loop(0, NG, unpack)
    last_g()
    loop(0, 4, hidden_and_pass)
    last_d(0)
    multiply(0, pass_more)
    send_back(0, pass_most)
    loop(N - NQ // 2, N, relay_d)
    last_d(1)
    multiply(1, nothing)
    send_back(1, nothing)
    collect(0)
    collect(1)
    for j in range(0, NB, 2):
        combine((j, j + 1))
        deliver(j).start()
        deliver(j + 1).start()
    for j in range(NB):
        deliver(j).wait()

    def left(ref, size, s):
        view = ref.at[pl.ds(0, size)]
        copy(view, view, s, sL, above).wait_send()

    left(WG, N - 1, sG)
    left(WG, 3 * N, sGY)
    left(WD, N - 1, sD)
    left(WD, 3 * N, sDY)
    left(SB, N - 1, sT)
    left(OB, 2 * N - 2, sO)


def permutation():
    p = np.zeros((NB * ROWS, GRP * ROWS), np.float32)
    for a in range(GRP):
        for j in range(NB):
            for r in range(CAP):
                p[a * ROWS + j * CAP + r, j * ROWS + a * CAP + r] = 1.0
    return p


def weaving():
    p = np.zeros((HALF, HALF), np.float32)
    for core in range(2):
        for s in range(8):
            for i in range(16):
                p[core * 128 + s * 16 + i, s * 32 + core * 16 + i] = 1.0
    return p


def shards(tokens, routes, router_weight, shift, scale, gate_mod, gate_weight, up_weight, down_weight):
    rows, width = tokens.shape
    perm, weave = jnp.asarray(permutation(), BF16), jnp.asarray(weaving(), BF16)
    small = (tokens, routes.T, router_weight.T, shift, scale, gate_mod, perm, weave)
    D = pltpu.SemaphoreType.DMA
    V = pltpu.VMEM
    hbm = pl.BlockSpec(memory_space=pl.ANY)
    return pl.pallas_call(
        kernel,
        name="experts",
        out_shape=jax.ShapeDtypeStruct((rows, width), BF16),
        in_specs=[hbm] * 11,
        out_specs=hbm,
        scratch_shapes=[V(a.shape, a.dtype) for a in small] + [
            V((NY * N, 2, 16, 1024), BF16),
            V((NY * N, 16, 1024), BF16),
            V((NB, rows, BLK), BF16),
            V((N, ROWS, BLK), BF16),
            V((N, ROWS, BLK), BF16),
            V((NB, N * CAP, BLK), BF16),
            V((N * CAP, 1024), BF16),
            V((NB, N * CAP, HALF), BF16),
            V((2 * N, ROWS, HALF), BF16),
            V((2 * N, ROWS, HALF), BF16),
            V((2 * NB, rows, HALF), F32),
            V((NG, 2 * rows, ROWS), BF16),
            V((2, rows, 128), F32),
            V((NB, BLK), F32),
            V((rows, width), BF16),
        ] + [D] * 7 + [D((N,)), D((N + 3,)), D((N,)), D((N + 6,))] + [D((NG,)), D((2 * NG,)), D((8,)), D((NB,))],
        compiler_params=pltpu.CompilerParams(
            collective_id=0, has_side_effects=True, vmem_limit_bytes=63 * 2**20
        ),
    )(*small, gate_weight, up_weight, down_weight)


def solution(mesh):
    spread = ("dp", "expert")
    in_specs = (
        P(spread, None), P(spread, None), P(), P(), P(), P(),
        P(None, spread, None), P(None, spread, None), P(None, spread, None),
    )
    return jax.shard_map(shards, mesh=mesh, in_specs=in_specs, out_specs=P(spread, None), check_vma=False)
```

```python
import functools

import jax
import jax.numpy as jnp
import numpy as np
from jax import lax
from jax.experimental import pallas as pl
from jax.experimental.pallas import tpu as pltpu
from jax.sharding import PartitionSpec as P

MESH = pl.DeviceIdType.MESH
PIX = 4096
EPS = 1e-06
NX, NZ, NC, NY = 4, 8, 2, 4
N = NX * NZ * NC
CAP = 6
BLK = 512
NB = 8
ROWS = NB * CAP
GRP = 8
NG = N // GRP
HALF = 256
NQ = NX * NZ
LAG = 4
ROT = 20
F32, BF16 = jnp.float32, jnp.bfloat16


def place(k):
    q = lax.rem(k + ROT, NQ)
    a, m = lax.div(q, 8), lax.rem(q, 8)
    dz = lax.rem(m * 7 + 4, NZ)
    dx = lax.rem(a + 2 * m + lax.div(m, 2), NX)
    return dx, dz, lax.div(k, NQ)


def kernel(
    tok_hbm, routes_hbm, router_hbm, shift_hbm, scale_hbm, gmod_hbm, perm_hbm, weave_hbm,
    gate, up, down, out,
    tok, routes, router, shift, scale, gmod, perm, weave, WG, WD, NBUF, SB, RB, XB, H, OUT, OB, IB, ACC, PICK, SCORE, GP, DONE,
    sG, sGY, sD, sDY, sT, sO, sL, rG, rGY, rD, rDY, rT, rO, sI, sE,
):
    e = lax.axis_index("expert")
    y = lax.axis_index("dp")
    x, z, c = lax.div(e, NZ * NC), lax.rem(lax.div(e, NC), NZ), lax.rem(e, NC)
    yp, ym, y2 = lax.rem(y + 1, NY), lax.rem(y + 3, NY), lax.rem(y + 2, NY)
    above, below = (yp, e), (ym, e)

    def chip(dx, dz):
        return lax.rem(x + dx, NX) * NZ + lax.rem(z + dz, NZ)

    def tgt(k):
        dx, dz, dc = place(k)
        return chip(dx, dz) * NC + lax.rem(c + dc, NC)

    def src(k):
        dx, dz, dc = place(k)
        return chip(NX - dx, NZ - dz) * NC + lax.rem(c + dc, NC)

    def loop(lo, hi, f):
        def body(k, carry):
            f(k)
            return carry
        lax.fori_loop(lo, hi, body, 0)

    def copy(a, b, s, r, device):
        return pltpu.make_async_remote_copy(a, b, s, r, device_id=device, device_id_type=MESH)

    bar = pltpu.get_barrier_semaphore()

    along_x = [lax.rem(x + d, NX) * (NZ * NC) for d in range(NX)]
    along_z = [lax.rem(z + d, NZ) * NC for d in range(NZ)]
    along_c = [lax.rem(c + d, NC) for d in range(NC)]
    for dz in (4, 3, 5, 2, 6, 1, 7, 0):
        for dx in (2, 1, 3, 0):
            for dc in range(NC):
                if dz or dx or dc:
                    there = along_x[dx] + along_z[dz] + along_c[dc]
                    pl.semaphore_signal(bar, 1, device_id=(y, there), device_id_type=MESH)
    pl.semaphore_signal(bar, 1, device_id=above, device_id_type=MESH)
    pl.semaphore_signal(bar, 1, device_id=below, device_id_type=MESH)
    small = (
        (tok_hbm, tok), (routes_hbm, routes), (router_hbm, router), (shift_hbm, shift),
        (scale_hbm, scale), (gmod_hbm, gmod), (perm_hbm, perm), (weave_hbm, weave),
    )
    loads = [pltpu.make_async_copy(a, b, sI.at[i]) for i, (a, b) in enumerate(small)]
    for load in loads:
        load.start()
    pl.semaphore_wait(bar, N + 1)

    def send_g(k):
        t = tgt(k)
        copy(gate.at[t], WG.at[y * N + e, 0], sG, rG.at[k], (y, t)).start()
        copy(up.at[t], WG.at[y * N + e, 1], sG, rG.at[k], (y, t)).start()

    mine_g = WG.at[y * N + e]
    mine_d = WD.at[c * NY * NQ + y * NQ + lax.div(e, NC)]
    pltpu.make_async_copy(gate.at[e], WG.at[y * N + e, 0], sL).start()
    pltpu.make_async_copy(up.at[e], WG.at[y * N + e, 1], sL).start()
    loop(1, N, send_g)
    pltpu.make_async_copy(mine_g, mine_g, sL).wait()
    pltpu.make_async_copy(down.at[e], mine_d, sL).start()

    def send_d(k):
        t = tgt(k)
        copy(down.at[t], mine_d, sD, rD.at[k], (y, t)).start()

    loop(1, NQ, send_d)
    pltpu.make_async_copy(mine_d, mine_d, sL).wait()

    for load in loads:
        load.wait()
    count = tok.shape[0]
    image = lax.div((y * N + e) * count, PIX)
    square = jnp.zeros((count, 1), F32)
    for j in range(NB):
        v = tok[:, j * BLK:(j + 1) * BLK].astype(F32)
        square = square + jnp.sum(v * v, axis=-1, keepdims=True)
    inv = lax.rsqrt(square * (1.0 / (NB * BLK)) + EPS)
    logits = jnp.zeros((count, N), F32)
    for j in range(NB):
        cols = slice(j * BLK, (j + 1) * BLK)
        v = tok[:, cols].astype(F32)
        normed = v * inv * (1.0 + scale[pl.ds(image, 1), cols]) + shift[pl.ds(image, 1), cols]
        normed = normed.astype(BF16)
        NBUF[j] = normed
        logits = logits + lax.dot_general(
            normed, router[:, cols], (((1,), (1,)), ((), ())), preferred_element_type=F32
        )
    experts = lax.broadcasted_iota(jnp.int32, (count, N), 1)
    tall = jnp.concatenate([routes[...].astype(F32), jnp.zeros((6, count), F32)], axis=0).T
    named = [tall[:, k:k + 1].astype(jnp.int32) for k in range(2)]
    hot = [(experts == named[k]).astype(F32) for k in range(2)]
    before = (
        lax.broadcasted_iota(jnp.int32, (count, count), 1)
        < lax.broadcasted_iota(jnp.int32, (count, count), 0)
    ).astype(F32).astype(BF16)
    earlier = jnp.dot(before, (hot[0] + hot[1]).astype(BF16), preferred_element_type=F32)
    places = lax.broadcasted_iota(jnp.int32, (count, N * CAP), 1)
    near = lax.broadcasted_iota(jnp.int32, (count, ROWS), 1)
    both = None
    for k in range(2):
        r = named[k]
        ex, ez, ec = r >> 4, (r >> 1) & 7, r & 1
        dx, dz, dc = (ex - x + NX) & 3, (ez - z + NZ) & 7, (ec + c) & 1
        m = (dz * 7 + 4) & 7
        a = (dx - 2 * m - (m >> 1) + 32) & 3
        step = ((8 * a + m + NQ - ROT) & (NQ - 1)) + NQ * dc
        slot = jnp.sum(hot[k] * earlier, axis=-1, keepdims=True).astype(jnp.int32)
        spot = step * CAP + slot
        pick = (places == spot).astype(F32)
        for g in range(NG):
            PICK[g, k * count:(k + 1) * count, :] = (near == spot - g * ROWS).astype(F32).astype(BF16)
        both = pick if both is None else both + pick
        chosen = jnp.sum(hot[k] * logits, axis=-1, keepdims=True)
        SCORE[k] = jnp.broadcast_to(jax.nn.sigmoid(chosen), (count, 128))
    select = both.T.astype(BF16)

    def gather_rows(j):
        XB[j] = jnp.dot(select, NBUF[j], preferred_element_type=F32).astype(BF16)
    loop(0, NB, gather_rows)

    def clear(j):
        ACC[j] = jnp.zeros(ACC.shape[1:], F32)
    loop(0, NC * NB, clear)

    for j in range(NB):
        left = gmod[pl.ds(image, 1), j * BLK:(j + 1) * BLK]
        terms = []
        for _ in range(3):
            term = left.astype(BF16)
            terms.append(term.astype(F32))
            left = left - terms[-1]
        stack = jnp.concatenate(terms + [jnp.zeros((5, BLK), F32)], axis=0).astype(BF16)
        for q in range(2):
            moved = lax.dot_general(
                stack[:, q * HALF:(q + 1) * HALF], weave[...], (((1,), (1,)), ((), ())),
                preferred_element_type=F32,
            )
            moved = moved[0:1] + moved[1:2] + moved[2:3]
            for kind in range(NC):
                at = kind * HALF + q * 128
                GP[j:j + 1, at:at + 128] = moved[:, kind * 128:(kind + 1) * 128]

    def rows_of(g):
        return pl.ds(pl.multiple_of(g * ROWS, 16), ROWS)

    def turn(block):
        return jnp.dot(perm[...], block, preferred_element_type=F32).astype(BF16)

    def pack(g):
        block = turn(XB[:, rows_of(g), :].reshape(NB * ROWS, BLK))
        SB[pl.ds(g * GRP, GRP)] = block.reshape(GRP, ROWS, BLK)

    def unpack(g):
        block = turn(RB[pl.ds(g * GRP, GRP)].reshape(GRP * ROWS, BLK))
        XB[:, rows_of(g), :] = block.reshape(NB, ROWS, BLK)

    def send_t(k):
        copy(SB.at[k], RB.at[k], sT, rT.at[lax.div(k, GRP)], (y, tgt(k))).start()

    def above_slot(k, shared):
        return k + lax.rem(k, 2) * (shared + 1 - k)

    def below_slot(k, shared):
        return shared + lax.rem(k, 2) * (k - shared)

    def forward_g(k):
        w = WG.at[y * N + src(k)]
        copy(w, w, sGY, rGY.at[above_slot(k, N)], above).start()
        copy(w, w, sGY, rGY.at[below_slot(k, N)], below).start()

    def relay_g(k):
        def one():
            w = WG.at[ym * N + src(k)]
            copy(w, w, sGY, rGY.at[k], above).wait_recv()
            copy(w, w, sGY, rGY.at[N + 2], above).start()

        def two():
            w = WG.at[yp * N + src(k)]
            copy(w, w, sGY, rGY.at[k], below).wait_recv()
            copy(w, w, sGY, rGY.at[N + 2], below).start()

        lax.cond(lax.rem(k, 2) == 0, one, two)

    def arrived(ref, first, size, s):
        w = ref.at[pl.ds(first, size)]
        copy(w, w, sL, s, above).wait_recv()

    def last_g():
        arrived(WG, yp * N, N // 2, rGY.at[N])
        arrived(WG, ym * N, N // 2, rGY.at[N + 1])
        arrived(WG, y2 * N, N, rGY.at[N + 2])

    forward_g(0)

    def step_g(k):
        @pl.when(k <= NG)
        def _():
            pack(k - 1)

        @pl.when((k >= 3) & (k < NG + 3))
        def _():
            first = (k - 3) * GRP
            loop(first, first + GRP, some_t)

        @pl.when(k == NG + 3)
        def _():
            loop(NQ, N, send_d)

        w = WG.at[y * N + src(k)]
        copy(w, w, sG, rG.at[k], above).wait_recv()
        forward_g(k)

        @pl.when(k >= LAG)
        def _():
            relay_g(k - LAG)

    def some_t(k):
        @pl.when(k > 0)
        def _():
            send_t(k)

    loop(1, N, step_g)
    loop(N - LAG, N, relay_g)
    RB[0] = SB[0]

    def class_of(phase):
        return lax.rem(c + phase, NC)

    def down_at(plane, k):
        return WD.at[class_of(lax.div(k, NQ)) * NY * NQ + plane * NQ + lax.div(src(k), NC)]

    def forward_d(k):
        w = down_at(y, k)

        @pl.when(k > 0)
        def _():
            copy(w, w, sD, rD.at[k], above).wait_recv()

        shared = N + 3 * lax.div(k, NQ)
        copy(w, w, sDY, rDY.at[above_slot(k, shared)], above).start()
        copy(w, w, sDY, rDY.at[below_slot(k, shared)], below).start()

    def relay_d(k):
        shared = N + 3 * lax.div(k, NQ)

        def one():
            w = down_at(ym, k)
            copy(w, w, sDY, rDY.at[k], above).wait_recv()
            copy(w, w, sDY, rDY.at[shared + 2], above).start()

        def two():
            w = down_at(yp, k)
            copy(w, w, sDY, rDY.at[k], below).wait_recv()
            copy(w, w, sDY, rDY.at[shared + 2], below).start()

        lax.cond(lax.rem(k, 2) == 0, one, two)

    def last_d(phase):
        first, shared = class_of(phase) * NY * NQ, N + 3 * phase
        arrived(WD, first + yp * NQ, NQ // 2, rDY.at[shared])
        arrived(WD, first + ym * NQ, NQ // 2, rDY.at[shared + 1])
        arrived(WD, first + y2 * NQ, NQ, rDY.at[shared + 2])

    def step_d(k):
        forward_d(k)

        @pl.when(k >= LAG)
        def _():
            relay_d(k - LAG)

    def hidden(n):
        cols = pl.ds(pl.multiple_of(n * 256, 256), 256)
        g = u = None
        for j in range(NB):
            rows = slice(j * 32, (j + 1) * 32)
            a = XB[j]
            pg = jnp.dot(a, WG[rows, 0, :, cols].reshape(BLK, 256), preferred_element_type=F32)
            pu = jnp.dot(a, WG[rows, 1, :, cols].reshape(BLK, 256), preferred_element_type=F32)
            g, u = (pg, pu) if g is None else (g + pg, u + pu)
        H[:, cols] = (g / (1.0 + jnp.exp(-g)) * u).astype(BF16)

    def send_o(kind, k):
        copy(
            OB.at[kind * N + k], IB.at[kind * N + k], sO,
            rO.at[kind * NG + lax.div(k, GRP)], (y, src(k)),
        ).start()

    def multiply(phase, also):
        kind = class_of(phase)

        def block(j):
            wd = WD[pl.ds(kind * NY * NQ + j * 16, 16)].reshape(HALF, 1024)
            o = lax.dot_general(H[...], wd, (((1,), (1,)), ((), ())), preferred_element_type=F32)
            OUT[j] = o.astype(BF16)
            also(j)
        loop(0, NB, block)

    def send_back(phase, also):
        kind = class_of(phase)

        def group(g):
            block = turn(OUT[:, rows_of(g), :].reshape(NB * ROWS, HALF))
            OB[pl.ds(kind * N + g * GRP, GRP)] = block.reshape(GRP, ROWS, HALF)

            @pl.when(g > 0)
            def _():
                loop(g * GRP - GRP, g * GRP, some)

            also(g)

        def some(k):
            @pl.when(k > 0)
            def _():
                send_o(kind, k)

        loop(0, NG, group)
        loop(N - GRP, N, some)
        IB[kind * N] = OB[kind * N]

    def collect(phase):
        def group(g):
            kind = lax.rem(c + phase + lax.div(g, NG // 2), NC)

            def wait(first, size):
                there = IB.at[pl.ds(kind * N + first, size)]
                copy(there, there, sO, rO.at[kind * NG + g], above).wait_recv()

            lax.cond(g == 0, lambda: wait(1, GRP - 1), lambda: wait(g * GRP, GRP))
            block = turn(IB[pl.ds(kind * N + g * GRP, GRP)].reshape(GRP * ROWS, HALF))
            for j in range(NB):
                rows = jnp.dot(PICK[g], block[j * ROWS:(j + 1) * ROWS], preferred_element_type=F32)
                total = rows[:count] * SCORE[0][:, 0:1] + rows[count:] * SCORE[1][:, 0:1]
                ACC[kind * NB + j] = ACC[kind * NB + j] + total
        loop(0, NG, group)

    def deliver(j):
        cols = slice(j * BLK, (j + 1) * BLK)
        return pltpu.make_async_copy(DONE.at[:, cols], out.at[:, cols], sE.at[j])

    def combine(some):
        stack = []
        for j in some:
            halves = [slice(kind * HALF, (kind + 1) * HALF) for kind in range(NC)]
            parts = [(GP[j:j + 1, halves[kind]] * ACC[kind * NB + j]).astype(BF16) for kind in range(NC)]
            for q in range(2):
                stack.append(jnp.concatenate([part[:, q * 128:(q + 1) * 128] for part in parts], axis=1))
        rows = jnp.dot(jnp.concatenate(stack, axis=0), weave[...], preferred_element_type=F32).astype(BF16)
        for i, j in enumerate(some):
            for q in range(2):
                at, row = j * BLK + q * HALF, (2 * i + q) * count
                DONE[:, at:at + HALF] = rows[row:row + count]

    def hidden_and_pass(n):
        hidden(n)
        loop(NQ + 4 * n, NQ + 4 * n + 4, forward_d)

    def pass_more(j):
        forward_d(NQ + 16 + j)
        relay_d(NQ + j)

    def pass_most(g):
        forward_d(NQ + 24 + g)
        relay_d(NQ + 8 + g)

    def nothing(_):
        pass

    loop(0, NQ, step_d)
    loop(NQ - LAG, NQ, relay_d)
    for g in range(NG):
        there = RB.at[pl.ds(max(1, g * GRP), GRP - (g == 0))]
        copy(there, there, sT, rT.at[g], above).wait_recv()
    loop(0, NG, unpack)
    last_g()
    loop(0, 4, hidden_and_pass)
    last_d(0)
    multiply(0, pass_more)
    send_back(0, pass_most)
    loop(N - NQ // 2, N, relay_d)
    last_d(1)
    multiply(1, nothing)
    send_back(1, nothing)
    collect(0)
    def left(ref, size, s):
        view = ref.at[pl.ds(0, size)]
        copy(view, view, s, sL, above).wait_send()

    left(WG, N - 1, sG)
    left(WG, 3 * N, sGY)
    left(WD, N - 1, sD)
    left(WD, 3 * N, sDY)
    left(SB, N - 1, sT)
    collect(1)
    for j in range(0, NB, 2):
        combine((j, j + 1))
        deliver(j).start()
        deliver(j + 1).start()
    for j in range(NB):
        deliver(j).wait()

    left(OB, 2 * N - 2, sO)


def permutation():
    p = np.zeros((NB * ROWS, GRP * ROWS), np.float32)
    for a in range(GRP):
        for j in range(NB):
            for r in range(CAP):
                p[a * ROWS + j * CAP + r, j * ROWS + a * CAP + r] = 1.0
    return p


def weaving():
    p = np.zeros((HALF, HALF), np.float32)
    for core in range(2):
        for s in range(8):
            for i in range(16):
                p[core * 128 + s * 16 + i, s * 32 + core * 16 + i] = 1.0
    return p


def shards(tokens, routes, router_weight, shift, scale, gate_mod, gate_weight, up_weight, down_weight):
    rows, width = tokens.shape
    perm, weave = jnp.asarray(permutation(), BF16), jnp.asarray(weaving(), BF16)
    small = (tokens, routes.T, router_weight.T, shift, scale, gate_mod, perm, weave)
    D = pltpu.SemaphoreType.DMA
    V = pltpu.VMEM
    hbm = pl.BlockSpec(memory_space=pl.ANY)
    return pl.pallas_call(
        kernel,
        name="experts",
        out_shape=jax.ShapeDtypeStruct((rows, width), BF16),
        in_specs=[hbm] * 11,
        out_specs=hbm,
        scratch_shapes=[V(a.shape, a.dtype) for a in small] + [
            V((NY * N, 2, 16, 1024), BF16),
            V((NY * N, 16, 1024), BF16),
            V((NB, rows, BLK), BF16),
            V((N, ROWS, BLK), BF16),
            V((N, ROWS, BLK), BF16),
            V((NB, N * CAP, BLK), BF16),
            V((N * CAP, 1024), BF16),
            V((NB, N * CAP, HALF), BF16),
            V((2 * N, ROWS, HALF), BF16),
            V((2 * N, ROWS, HALF), BF16),
            V((2 * NB, rows, HALF), F32),
            V((NG, 2 * rows, ROWS), BF16),
            V((2, rows, 128), F32),
            V((NB, BLK), F32),
            V((rows, width), BF16),
        ] + [D] * 7 + [D((N,)), D((N + 3,)), D((N,)), D((N + 6,))] + [D((NG,)), D((2 * NG,)), D((8,)), D((NB,))],
        compiler_params=pltpu.CompilerParams(
            collective_id=0, has_side_effects=True, vmem_limit_bytes=63 * 2**20
        ),
    )(*small, gate_weight, up_weight, down_weight)


def solution(mesh):
    spread = ("dp", "expert")
    in_specs = (
        P(spread, None), P(spread, None), P(), P(), P(), P(),
        P(None, spread, None), P(None, spread, None), P(None, spread, None),
    )
    return jax.shard_map(shards, mesh=mesh, in_specs=in_specs, out_specs=P(spread, None), check_vma=False)
```
